32 devices in a mesh: mats: 8 (over z, x), tp: 4 (over y, core).
Axes of the slice: x: 2, y: 2, z: 4, core: 2. Of those that a mesh axis runs over, the one named last changes fastest.
Arguments:
- grad: bfloat16 [3072, 16384], P('tp', 'mats'), may hold values from -40 to 40
- momentum: float32 [3072, 16384], P('tp', 'mats'), may hold values from -6 to 6
Outputs:
- update: bfloat16 [3072, 16384], P('tp', 'mats')
- new_momentum: float32 [3072, 16384], P('tp', 'mats')
The draws below stay inside these ranges and needn't reach their ends.
All inputs are finite; a program needn't handle non-finite values.
Results may differ from the reference program's by a relative error of at most 0.01.
Values may be sent and summed in bfloat16 or wider, within the bound.
A program may use at most 128 MiB of HBM per device.

```python
import math
import jax
import jax.numpy as jnp
from jax import lax

R = 3072
C = 16384
ITERS = 2


def draw_grad(key, part):
    keys = jax.random.split(jax.random.fold_in(key, 11), 3)
    position = jnp.arange(R, dtype=jnp.float32).reshape(R, 1) / (R - 1.0)
    rising = jnp.exp(math.log(0.1) * (1.0 - position))
    rough_rows = jax.random.uniform(keys[0], (R, 1), jnp.float32, 0.5, 1.0)
    row_scale = rising * rough_rows
    col_scale = jnp.exp(jax.random.uniform(keys[1], (1, C), jnp.float32, 0.0, math.log(10.0)))
    base = jax.random.normal(keys[2], (R, C), jnp.float32)
    base = jnp.clip(base, -4.0, 4.0)
    return (base * row_scale * col_scale).astype(jnp.bfloat16)


def level_of(own_key, extent, shards, low, largest):
    loudness = 1.0
    for dim, shards_of in shards:
        heights = jax.random.uniform(jax.random.fold_in(jax.random.fold_in(own_key, 6), dim), (shards_of,), jnp.float32, low / len(shards), largest / len(shards))
        loudness = loudness * jnp.repeat(jnp.exp(heights), extent[dim] // shards_of).reshape((-1,) + (1,) * (len(extent) - 1 - dim))
    return loudness


def normal_values(key, extent, width, reach, cuts=(), held_as=jnp.bfloat16):
    entries = width * jax.random.normal(key, extent, jnp.float32)
    if cuts:
        entries = entries * level_of(key, extent, cuts, -0.22, 0.18)
    return jnp.clip(entries, -reach, reach).astype(held_as)


def setup_inputs(seed: int = 0) -> dict:
    key_of = jax.random.split(jax.random.key(seed), 3)
    grad = draw_grad(jax.random.fold_in(key_of[2], 71), 0)
    momentum = normal_values(key_of[1], (R, C), 1.0, 6.0, ((0, 4), (1, 8)), jnp.float32)
    return {"grad": grad, "momentum": momentum}


momentum_beta = 0.95
first_coef = 3.4445
second_coef = -4.775
third_coef = 2.0315
shape_gain = 0.2
epsilon = 1e-06

def reference(grad, momentum):
    new_momentum = momentum_beta * momentum + grad.astype(jnp.float32)
    iterate = (grad.astype(jnp.float32) + momentum_beta * new_momentum).astype(jnp.bfloat16)
    for step in range(ITERS):
        gram = lax.dot_general(iterate, iterate, (((1,), (1,)), ((), ())), preferred_element_type=jnp.float32).astype(jnp.bfloat16)
        first = jnp.dot(gram, iterate, preferred_element_type=jnp.float32).astype(jnp.bfloat16)
        second = jnp.dot(gram, first, preferred_element_type=jnp.float32).astype(jnp.bfloat16)
        if step == 0:
            bound = jnp.max(lax.optimization_barrier(jnp.sum(jnp.abs(gram.astype(jnp.float32)), axis=1))) + epsilon
            root = lax.rsqrt(bound)
            mixed = first_coef * iterate.astype(jnp.float32) * root + second_coef * first.astype(jnp.float32) * root ** 3 + third_coef * second.astype(jnp.float32) * root ** 5
        else:
            mixed = first_coef * iterate.astype(jnp.float32) + second_coef * first.astype(jnp.float32) + third_coef * second.astype(jnp.float32)
        iterate = mixed.astype(jnp.bfloat16)
    update = (shape_gain * math.sqrt(max(R, C)) * iterate.astype(jnp.float32)).astype(jnp.bfloat16)
    return (update, new_momentum)
```

```python
import functools
import math

import jax
import jax.numpy as jnp
from jax import lax
from jax.experimental import pallas as pl
from jax.experimental.pallas import tpu as pltpu
from jax.sharding import PartitionSpec as P

momentum_beta = 0.95
first_coef = 3.4445
second_coef = -4.775
third_coef = 2.0315
shape_gain = 0.2
epsilon = 1e-06
grant = 62 * 1024 * 1024


def nt_dot(left, right):
    return lax.dot_general(
        left, right, (((1,), (1,)), ((), ())), preferred_element_type=jnp.float32
    )


def window_of(blocks):
    return blocks // 2 + 1


def gram_kernel(block, where_ref, x_ref, part_ref):
    blocks = x_ref.shape[0] // block
    mine = part_ref.shape[0] // block
    window = part_ref.shape[1] // block
    first = where_ref[0] * mine
    left_at = pl.ds(pl.multiple_of(first * block, block), mine * block)
    for j in range(mine + window - 1):
        low, high = max(0, j - window + 1), min(mine - 1, j)
        other = lax.rem(first + j, blocks)
        right = x_ref[pl.ds(pl.multiple_of(other * block, block), block), :]
        rows = pl.ds(
            pl.multiple_of((first + low) * block, block), (high - low + 1) * block
        )
        product = nt_dot(x_ref[rows, :], right).astype(jnp.bfloat16)
        for i in range(low, high + 1):
            at = (i - low) * block
            part_ref[i * block : (i + 1) * block, (j - i) * block : (j - i + 1) * block] = (
                product[at : at + block, :]
            )


def poly_kernel(block, scale, where_ref, compact_ref, out_ref, kappa_ref, gram, own, one, two, left, right):
    size = gram.shape[0]
    blocks = size // block
    window = compact_ref.shape[1] // block
    for i in range(blocks):
        for d in range(window):
            j = (i + d) % blocks
            tile = compact_ref[i * block : (i + 1) * block, d * block : (d + 1) * block]
            gram[i * block : (i + 1) * block, j * block : (j + 1) * block] = tile
            if d > 0 and 2 * d != blocks:
                gram[j * block : (j + 1) * block, i * block : (i + 1) * block] = tile.T

    def column_sums(step, total):
        rows = jnp.abs(gram[pl.ds(pl.multiple_of(step * 16, 16), 16), :].astype(jnp.float32))
        return total + (rows[0:8] + rows[8:16])

    total = lax.fori_loop(0, size // 16, column_sums, jnp.zeros((8, size), jnp.float32))
    bound = jnp.max(jnp.sum(total, axis=0, keepdims=True), axis=1, keepdims=True) + epsilon
    root = lax.rsqrt(jnp.broadcast_to(bound, (1, 128)))
    kappa = (scale * first_coef * first_coef) * root
    kappa_ref[...] = kappa
    inverse = (root * root)[:, :1]
    count = own.shape[0]
    width = math.gcd(size, 1024)

    def columns(body):
        @pl.loop(0, size // width)
        def _(step):
            body(pl.ds(pl.multiple_of(step * width, width), width))

    def times_gram(source, at):
        return inverse * jnp.dot(source[...], gram[:, at], preferred_element_type=jnp.float32)

    def wide(ref, at):
        return ref[:, at].astype(jnp.float32)

    def apply(source, target, constant=None):
        def body(at):
            value = times_gram(source, at)
            if constant is not None:
                value = value + (constant * inverse) * wide(own, at)
            target[:, at] = value.astype(jnp.bfloat16)

        columns(body)

    def polynomial(source, middle, target):
        apply(source, middle)

        def body(at):
            target[:, at] = (
                first_coef * wide(source, at)
                + second_coef * wide(middle, at)
                + third_coef * times_gram(middle, at)
            ).astype(jnp.bfloat16)

        columns(body)

    if count % 16 == 0:
        own[...] = gram[pl.ds(pl.multiple_of(where_ref[0] * count, 16), count), :]
    else:
        row = lax.broadcasted_iota(jnp.int32, (count, size), 0) + where_ref[0] * count
        column = lax.broadcasted_iota(jnp.int32, (count, size), 1)
        two[...] = (row == column).astype(jnp.float32).astype(jnp.bfloat16)

        def select(at):
            own[:, at] = jnp.dot(
                two[...], gram[:, at], preferred_element_type=jnp.float32
            ).astype(jnp.bfloat16)

        columns(select)

    def start(at):
        left[:, at] = (inverse * wide(own, at)).astype(jnp.bfloat16)

    columns(start)

    def first(at):
        one[:, at] = (
            second_coef * wide(left, at) + third_coef * times_gram(left, at)
        ).astype(jnp.bfloat16)

    columns(first)
    apply(one, left, first_coef)
    polynomial(left, right, two)
    polynomial(two, right, left)

    def keep(at):
        two[:, at] = left[:, at]

    columns(keep)
    apply(two, right)
    polynomial(right, left, own)
    polynomial(own, left, right)

    def finish(at):
        mixed = (
            first_coef * wide(one, at) + second_coef * wide(two, at) + third_coef * wide(right, at)
        )
        out_ref[:, at] = ((scale * root[:, :1]) * mixed).astype(jnp.bfloat16)

    columns(finish)


def per_device(scale, grad, momentum):
    new_momentum = momentum_beta * momentum + grad.astype(jnp.float32)
    iterate = (grad.astype(jnp.float32) + momentum_beta * new_momentum).astype(jnp.bfloat16)
    columns = lax.all_gather(iterate, "tp", axis=0, tiled=True)
    size = columns.shape[0]
    mine = iterate.shape[0]
    block = math.gcd(mine, 256)
    window = window_of(size // block) * block
    smem = pl.BlockSpec(memory_space=pltpu.SMEM)
    whole = pl.BlockSpec(memory_space=pltpu.VMEM)
    params = pltpu.CompilerParams(vmem_limit_bytes=grant)
    tp = lax.axis_index("tp")
    part = pl.pallas_call(
        functools.partial(gram_kernel, block),
        out_shape=jax.ShapeDtypeStruct((mine, window), jnp.bfloat16),
        in_specs=[smem, whole],
        out_specs=whole,
        compiler_params=params,
        name="gram",
    )(tp.reshape(1), columns)
    share = lax.psum_scatter(part, "mats", scatter_dimension=0, tiled=True)
    compact = lax.all_gather(share, ("tp", "mats"), axis=0, tiled=True)
    count = share.shape[0]
    place = tp * lax.axis_size("mats") + lax.axis_index("mats")
    thin = pltpu.VMEM((count, size), jnp.bfloat16)
    rows, kappa = pl.pallas_call(
        functools.partial(poly_kernel, block, scale),
        out_shape=(
            jax.ShapeDtypeStruct((count, size), jnp.bfloat16),
            jax.ShapeDtypeStruct((1, 128), jnp.float32),
        ),
        in_specs=[smem, whole],
        out_specs=(whole, whole),
        scratch_shapes=[pltpu.VMEM((size, size), jnp.bfloat16)] + [thin] * 5,
        compiler_params=params,
        cost_estimate=pl.CostEstimate(
            flops=22 * count * size * size, bytes_accessed=size * window * 2, transcendentals=0
        ),
        name="poly",
    )(place.reshape(1), compact)
    matrix = lax.all_gather(rows, "mats", axis=0, tiled=True)
    product = jnp.dot(matrix, columns, preferred_element_type=jnp.float32)
    update = (product + kappa[0, 0] * iterate.astype(jnp.float32)).astype(jnp.bfloat16)
    return (update, new_momentum)


def solution(mesh):
    def step(grad, momentum):
        scale = shape_gain * math.sqrt(max(grad.shape))
        return jax.shard_map(
            functools.partial(per_device, scale),
            mesh=mesh,
            in_specs=(P("tp", "mats"), P("tp", "mats")),
            out_specs=(P("tp", "mats"), P("tp", "mats")),
            check_vma=False,
        )(grad, momentum)

    return step
```

```python
import functools
import math

import jax
import jax.numpy as jnp
from jax import lax
from jax.experimental import pallas as pl
from jax.experimental.pallas import tpu as pltpu
from jax.sharding import PartitionSpec as P

momentum_beta = 0.95
first_coef = 3.4445
second_coef = -4.775
third_coef = 2.0315
shape_gain = 0.2
epsilon = 1e-06
grant = 62 * 1024 * 1024


def digits_of(mesh):
    table = {}
    shape = mesh.devices.shape
    for number, axis in enumerate(mesh.axis_names):
        extent = shape[number]
        line = [mesh.devices[tuple(i if k == number else 0 for k in range(len(shape)))] for i in range(extent)]
        found = []
        if all(hasattr(device, "coords") for device in line):
            places = [(*device.coords, device.core_on_chip) for device in line]
            for place, column in enumerate(zip(*places)):
                kinds = len(set(column))
                if kinds > 1:
                    stride = next(i for i in range(extent) if column[i] != column[0])
                    if all((i // stride) % kinds == column[i] - column[0] for i in range(extent)):
                        found.append((axis, stride, kinds, place == 3))
        if math.prod(kinds for _, _, kinds, _ in found) != extent:
            found = [(axis, 1, extent, False)]
        table[axis] = sorted(found, key=lambda digit: -digit[1])
    return table


def place(digit):
    axis, stride, extent, _ = digit
    return lax.rem(lax.div(lax.axis_index(axis), stride), extent)


def moves(digit):
    here, extent = place(digit), digit[2]
    if extent == 2:
        return [(1 - 2 * here, None)]
    return [(1, here + 1 < extent), (-1, here >= 1)]


def when(condition, body):
    if condition is None:
        body()
    else:
        pl.when(condition)(body)


def both(*conditions):
    found = [c for c in conditions if c is not None]
    return functools.reduce(lambda a, b: a & b, found) if found else None


def peer(digit, offset):
    axis, stride, _, _ = digit
    return {axis: lax.axis_index(axis) + offset * stride}


def barrier_all(digits):
    semaphore = pltpu.get_barrier_semaphore()
    for digit in digits:
        for offset, has in moves(digit):
            when(has, functools.partial(
                pl.semaphore_signal, semaphore, inc=1, device_id=peer(digit, offset),
                device_id_type=pl.DeviceIdType.MESH))
    count = 0
    for digit in digits:
        for _, has in moves(digit):
            count = count + (1 if has is None else has.astype(jnp.int32))
    pl.semaphore_wait(semaphore, count)


def relatives(digit):
    here, extent = place(digit), digit[2]
    if extent == 2:
        return [(1, 2 * here - 1, 1 - here, None)]
    found = []
    for hop in range(1, extent):
        found.append((hop, 1, here - hop, here >= hop))
        found.append((hop, -1, here + hop, here + hop < extent))
    return found


class Gather:
    def __init__(self, layout, pieces, buffer, source, send_sem, recv_sem):
        self.layout, self.pieces, self.buffer, self.source = layout, pieces, buffer, source
        self.send_sem, self.recv_sem = send_sem, recv_sem
        self.sent = []

    @staticmethod
    def semaphores(layout, pieces):
        dims = tuple(d[2] for d in layout)
        return [
            pltpu.SemaphoreType.DMA((len(pieces), 2 * len(layout)) + dims),
            pltpu.SemaphoreType.DMA((len(pieces),) + dims),
        ]

    def copy(self, piece, block, digit, offset, way, own):
        order, row, count = self.pieces[piece]
        index = tuple(block[d] for d in self.layout)
        rows = (pl.ds(row, count), slice(None))
        at = self.buffer.at[index + rows]
        lane = 2 * self.layout.index(digit) + way
        return pltpu.make_async_remote_copy(
            src_ref=self.source.at[rows] if own else at,
            dst_ref=at,
            send_sem=self.send_sem.at[(piece, lane) + index],
            recv_sem=self.recv_sem.at[(piece,) + index],
            device_id=peer(digit, offset),
            device_id_type=pl.DeviceIdType.MESH,
        )

    def send(self, piece, block, exists, digit, directions, own=False):
        for way, (offset, has) in enumerate(moves(digit)):
            if directions is not None and way not in directions:
                continue
            copy = self.copy(piece, block, digit, offset, way, own)
            condition = both(exists, has)
            when(condition, copy.start)
            self.sent.append((condition, copy))

    def events(self, piece):
        order = self.pieces[piece][0]
        here = {d: place(d) for d in order}
        found = []

        def begin(after):
            for digit in order:
                self.send(piece, here, None, digit, None, own=True)

        found.append((0, begin))

        def arrivals(stage, block, exists, depth):
            digit = order[stage]
            for hop, travel, q, there in relatives(digit):
                source = {**block, digit: q}
                condition = both(exists, there)

                def arrive(after, stage=stage, digit=digit, source=source, condition=condition, hop=hop, travel=travel):
                    offset, _ = moves(digit)[0]
                    when(condition, self.copy(piece, source, digit, offset, 0, False).wait_recv)
                    if digit[2] > 2:
                        self.send(piece, source, condition, digit, (0 if travel > 0 else 1,))
                    for later in order[stage + 1 :]:
                        self.send(piece, source, condition, later, None)
                    if after is not None:
                        after(piece, source, condition)

                found.append((depth + hop, arrive))

        def expand(stage, earlier, block, exists, depth):
            if earlier == stage:
                arrivals(stage, block, exists, depth)
                return
            digit = order[earlier]
            expand(stage, earlier + 1, {**block, digit: here[digit]}, exists, depth)
            for hop, _, q, there in relatives(digit):
                expand(stage, earlier + 1, {**block, digit: q}, both(exists, there), depth + hop)

        for stage in range(len(order)):
            expand(stage, 0, dict(here), None, 0)
        return found

    def run(self, after=None):
        queue = []
        for piece in range(len(self.pieces)):
            for depth, action in self.events(piece):
                queue.append((depth, piece, len(queue), action))
        for _, _, _, action in sorted(queue, key=lambda entry: entry[:3]):
            action(after)

    def drain(self):
        for condition, copy in self.sent:
            when(condition, copy.wait_send)


def gather_kernel(layout, pieces, x_ref, out_ref, send_sem, recv_sem, local_sem):
    barrier_all(layout)
    gather = Gather(layout, pieces, out_ref, x_ref, send_sem, recv_sem)
    gather.run()
    local = pltpu.make_async_copy(x_ref, out_ref.at[tuple(place(d) for d in layout)], local_sem)
    local.start()
    local.wait()
    gather.drain()


def pieces_of(rows, orders, chunks):
    units = max(1, rows // 16)
    chunks = min(chunks, units)
    cuts = [units * i // chunks * 16 for i in range(chunks)] + [rows]
    return [(orders[i % len(orders)], cuts[i], cuts[i + 1] - cuts[i]) for i in range(chunks)]


def events_of(order):
    total, held = 0, 1
    for digit in order:
        around = 1 if digit[2] == 2 else 2 * (digit[2] - 1)
        total += held * around
        held *= 1 + around
    return total


def gather(x, axes, layout, orders, chunks, ident, name):
    rows, columns = x.shape
    if rows % 16 or len(orders) * events_of(orders[0]) > 256:
        return lax.all_gather(x, axes, axis=0, tiled=True)
    pieces = pieces_of(rows, orders, chunks)
    dims = tuple(d[2] for d in layout)
    out = pl.pallas_call(
        functools.partial(gather_kernel, layout, pieces),
        out_shape=jax.ShapeDtypeStruct(dims + (rows, columns), x.dtype),
        in_specs=[pl.BlockSpec(memory_space=pltpu.VMEM)],
        out_specs=pl.BlockSpec(memory_space=pl.ANY),
        scratch_shapes=Gather.semaphores(layout, pieces) + [pltpu.SemaphoreType.DMA],
        compiler_params=pltpu.CompilerParams(collective_id=ident, has_side_effects=True),
        name=name,
    )(x)
    return out.reshape(math.prod(dims) * rows, columns)


def nt_dot(left, right):
    return lax.dot_general(
        left, right, (((1,), (1,)), ((), ())), preferred_element_type=jnp.float32
    )


def window_of(blocks):
    return blocks // 2 + 1


def gram_kernel(block, where_ref, x_ref, part_ref):
    blocks = x_ref.shape[0] // block
    mine = part_ref.shape[0] // block
    window = part_ref.shape[1] // block
    first = where_ref[0] * mine
    left_at = pl.ds(pl.multiple_of(first * block, block), mine * block)
    for j in range(mine + window - 1):
        low, high = max(0, j - window + 1), min(mine - 1, j)
        other = lax.rem(first + j, blocks)
        right = x_ref[pl.ds(pl.multiple_of(other * block, block), block), :]
        rows = pl.ds(
            pl.multiple_of((first + low) * block, block), (high - low + 1) * block
        )
        product = nt_dot(x_ref[rows, :], right).astype(jnp.bfloat16)
        for i in range(low, high + 1):
            at = (i - low) * block
            part_ref[i * block : (i + 1) * block, (j - i) * block : (j - i + 1) * block] = (
                product[at : at + block, :]
            )


def poly_kernel(block, scale, where_ref, compact_ref, out_ref, kappa_ref, gram, own, one, two, left, right):
    size = gram.shape[0]
    blocks = size // block
    window = compact_ref.shape[1] // block
    for i in range(blocks):
        for d in range(window):
            j = (i + d) % blocks
            tile = compact_ref[i * block : (i + 1) * block, d * block : (d + 1) * block]
            gram[i * block : (i + 1) * block, j * block : (j + 1) * block] = tile
            if d > 0 and 2 * d != blocks:
                gram[j * block : (j + 1) * block, i * block : (i + 1) * block] = tile.T

    def column_sums(step, total):
        rows = jnp.abs(gram[pl.ds(pl.multiple_of(step * 16, 16), 16), :].astype(jnp.float32))
        return total + (rows[0:8] + rows[8:16])

    total = lax.fori_loop(0, size // 16, column_sums, jnp.zeros((8, size), jnp.float32))
    bound = jnp.max(jnp.sum(total, axis=0, keepdims=True), axis=1, keepdims=True) + epsilon
    root = lax.rsqrt(jnp.broadcast_to(bound, (1, 128)))
    kappa = (scale * first_coef * first_coef) * root
    kappa_ref[...] = kappa
    inverse = (root * root)[:, :1]
    count = own.shape[0]
    width = math.gcd(size, 1024)

    def columns(body):
        @pl.loop(0, size // width)
        def _(step):
            body(pl.ds(pl.multiple_of(step * width, width), width))

    def times_gram(source, at):
        return inverse * jnp.dot(source[...], gram[:, at], preferred_element_type=jnp.float32)

    def wide(ref, at):
        return ref[:, at].astype(jnp.float32)

    def apply(source, target, constant=None):
        def body(at):
            value = times_gram(source, at)
            if constant is not None:
                value = value + (constant * inverse) * wide(own, at)
            target[:, at] = value.astype(jnp.bfloat16)

        columns(body)

    def polynomial(source, middle, target):
        apply(source, middle)

        def body(at):
            target[:, at] = (
                first_coef * wide(source, at)
                + second_coef * wide(middle, at)
                + third_coef * times_gram(middle, at)
            ).astype(jnp.bfloat16)

        columns(body)

    if count % 16 == 0:
        own[...] = gram[pl.ds(pl.multiple_of(where_ref[0] * count, 16), count), :]
    else:
        row = lax.broadcasted_iota(jnp.int32, (count, size), 0) + where_ref[0] * count
        column = lax.broadcasted_iota(jnp.int32, (count, size), 1)
        two[...] = (row == column).astype(jnp.float32).astype(jnp.bfloat16)

        def select(at):
            own[:, at] = jnp.dot(
                two[...], gram[:, at], preferred_element_type=jnp.float32
            ).astype(jnp.bfloat16)

        columns(select)

    def start(at):
        left[:, at] = (inverse * wide(own, at)).astype(jnp.bfloat16)

    columns(start)

    def first(at):
        one[:, at] = (
            second_coef * wide(left, at) + third_coef * times_gram(left, at)
        ).astype(jnp.bfloat16)

    columns(first)
    apply(one, left, first_coef)
    polynomial(left, right, two)
    polynomial(two, right, left)

    def keep(at):
        two[:, at] = left[:, at]

    columns(keep)
    apply(two, right)
    polynomial(right, left, own)
    polynomial(own, left, right)

    def finish(at):
        mixed = (
            first_coef * wide(one, at) + second_coef * wide(two, at) + third_coef * wide(right, at)
        )
        out_ref[:, at] = ((scale * root[:, :1]) * mixed).astype(jnp.bfloat16)

    columns(finish)


def orders_of(digits):
    layout = tuple(digits["tp"]) + tuple(digits["mats"])
    far = {axis: [d for d in found if not d[3]] for axis, found in digits.items()}
    near = [d for d in layout if d[3]]
    one = tuple(far["mats"] + far["tp"] + near)
    two = tuple(far["mats"][:1] + far["tp"] + far["mats"][1:] + near)
    return layout, [one, two] if one != two else [one]


def per_device(scale, digits, grad, momentum):
    new_momentum = momentum_beta * momentum + grad.astype(jnp.float32)
    iterate = (grad.astype(jnp.float32) + momentum_beta * new_momentum).astype(jnp.bfloat16)
    layout, orders = orders_of(digits)
    lines = {axis: tuple(sorted(found, key=lambda d: d[3])) for axis, found in digits.items()}
    columns = gather(iterate, "tp", tuple(digits["tp"]), [lines["tp"]], 6, 1, "gather_x")
    size = columns.shape[0]
    mine = iterate.shape[0]
    block = math.gcd(mine, 256)
    window = window_of(size // block) * block
    smem = pl.BlockSpec(memory_space=pltpu.SMEM)
    whole = pl.BlockSpec(memory_space=pltpu.VMEM)
    params = pltpu.CompilerParams(vmem_limit_bytes=grant)
    tp = lax.axis_index("tp")
    part = pl.pallas_call(
        functools.partial(gram_kernel, block),
        out_shape=jax.ShapeDtypeStruct((mine, window), jnp.bfloat16),
        in_specs=[smem, whole],
        out_specs=whole,
        compiler_params=params,
        name="gram",
    )(tp.reshape(1), columns)
    share = lax.psum_scatter(part, "mats", scatter_dimension=0, tiled=True)
    compact = gather(share, ("tp", "mats"), layout, orders, 2, 2, "gather_gram")
    count = share.shape[0]
    place = tp * lax.axis_size("mats") + lax.axis_index("mats")
    thin = pltpu.VMEM((count, size), jnp.bfloat16)
    rows, kappa = pl.pallas_call(
        functools.partial(poly_kernel, block, scale),
        out_shape=(
            jax.ShapeDtypeStruct((count, size), jnp.bfloat16),
            jax.ShapeDtypeStruct((1, 128), jnp.float32),
        ),
        in_specs=[smem, whole],
        out_specs=(whole, whole),
        scratch_shapes=[pltpu.VMEM((size, size), jnp.bfloat16)] + [thin] * 5,
        compiler_params=params,
        cost_estimate=pl.CostEstimate(
            flops=22 * count * size * size, bytes_accessed=size * window * 2, transcendentals=0
        ),
        name="poly",
    )(place.reshape(1), compact)
    matrix = gather(rows, "mats", tuple(digits["mats"]), [lines["mats"]], 3, 3, "gather_rows")
    product = jnp.dot(matrix, columns, preferred_element_type=jnp.float32)
    update = (product + kappa[0, 0] * iterate.astype(jnp.float32)).astype(jnp.bfloat16)
    return (update, new_momentum)


def solution(mesh):
    digits = digits_of(mesh)

    def step(grad, momentum):
        scale = shape_gain * math.sqrt(max(grad.shape))
        return jax.shard_map(
            functools.partial(per_device, scale, digits),
            mesh=mesh,
            in_specs=(P("tp", "mats"), P("tp", "mats")),
            out_specs=(P("tp", "mats"), P("tp", "mats")),
            check_vma=False,
        )(grad, momentum)

    return step
```

```python
import functools
import math

import jax
import jax.numpy as jnp
from jax import lax
from jax.experimental import pallas as pl
from jax.experimental.pallas import tpu as pltpu
from jax.sharding import PartitionSpec as P

momentum_beta = 0.95
first_coef = 3.4445
second_coef = -4.775
third_coef = 2.0315
shape_gain = 0.2
epsilon = 1e-06
grant = 62 * 1024 * 1024


def digits_of(mesh):
    table = {}
    shape = mesh.devices.shape
    for number, axis in enumerate(mesh.axis_names):
        extent = shape[number]
        line = [mesh.devices[tuple(i if k == number else 0 for k in range(len(shape)))] for i in range(extent)]
        found = []
        if all(hasattr(device, "coords") for device in line):
            places = [(*device.coords, device.core_on_chip) for device in line]
            for place, column in enumerate(zip(*places)):
                kinds = len(set(column))
                if kinds > 1:
                    stride = next(i for i in range(extent) if column[i] != column[0])
                    if all((i // stride) % kinds == column[i] - column[0] for i in range(extent)):
                        found.append((axis, stride, kinds, place == 3))
        if math.prod(kinds for _, _, kinds, _ in found) != extent:
            found = [(axis, 1, extent, False)]
        table[axis] = sorted(found, key=lambda digit: -digit[1])
    return table


def place(digit):
    axis, stride, extent, _ = digit
    return lax.rem(lax.div(lax.axis_index(axis), stride), extent)


def moves(digit):
    here, extent = place(digit), digit[2]
    if extent == 2:
        return [(1 - 2 * here, None)]
    return [(1, here + 1 < extent), (-1, here >= 1)]


def when(condition, body):
    if condition is None:
        body()
    else:
        pl.when(condition)(body)


def both(*conditions):
    found = [c for c in conditions if c is not None]
    return functools.reduce(lambda a, b: a & b, found) if found else None


def peer(digit, offset):
    axis, stride, _, _ = digit
    return {axis: lax.axis_index(axis) + offset * stride}


def barrier_all(digits):
    semaphore = pltpu.get_barrier_semaphore()
    for digit in digits:
        for offset, has in moves(digit):
            when(has, functools.partial(
                pl.semaphore_signal, semaphore, inc=1, device_id=peer(digit, offset),
                device_id_type=pl.DeviceIdType.MESH))
    count = 0
    for digit in digits:
        for _, has in moves(digit):
            count = count + (1 if has is None else has.astype(jnp.int32))
    pl.semaphore_wait(semaphore, count)


def around(digit, step):
    here = place(digit)
    there = lax.rem(here + step, digit[2])
    return there, there - here


def barrier_lines(digits):
    semaphore = pltpu.get_barrier_semaphore()
    count = 0
    for digit in digits:
        for step in range(1, digit[2]):
            _, offset = around(digit, step)
            pl.semaphore_signal(
                semaphore, inc=1, device_id=peer(digit, offset),
                device_id_type=pl.DeviceIdType.MESH,
            )
            count += 1
    pl.semaphore_wait(semaphore, count)


def relatives(digit):
    here, extent = place(digit), digit[2]
    if extent == 2:
        return [(1, 0, 1 - here, None)]
    found = []
    for hop in range(1, extent):
        found.append((hop, 1, here - hop, here >= hop))
        found.append((hop, -1, here + hop, here + hop < extent))
    return found


class Gather:
    def __init__(self, layout, pieces, buffer, source, send_sem, recv_sem):
        self.layout, self.pieces, self.buffer, self.source = layout, pieces, buffer, source
        self.send_sem, self.recv_sem = send_sem, recv_sem
        self.sent = {}

    @staticmethod
    def semaphores(layout, pieces):
        dims = tuple(d[2] for d in layout)
        return [
            pltpu.SemaphoreType.DMA((len(pieces), 2 * len(layout)) + dims),
            pltpu.SemaphoreType.DMA((len(pieces),) + dims),
        ]

    def copy(self, piece, block, digit, offset, way, own):
        order, row, count = self.pieces[piece]
        index = tuple(block[d] for d in self.layout)
        rows = (pl.ds(row, count), slice(None))
        at = self.buffer.at[index + rows]
        lane = 2 * self.layout.index(digit) + way
        return pltpu.make_async_remote_copy(
            src_ref=self.source.at[rows] if own else at,
            dst_ref=at,
            send_sem=self.send_sem.at[(piece, lane) + index],
            recv_sem=self.recv_sem.at[(piece,) + index],
            device_id=peer(digit, offset),
            device_id_type=pl.DeviceIdType.MESH,
        )

    def send(self, piece, block, exists, digit, directions, tag, own=False):
        for way, (offset, has) in enumerate(moves(digit)):
            if directions is not None and way not in directions:
                continue
            copy = self.copy(piece, block, digit, offset, way, own)
            condition = both(exists, has)
            when(condition, copy.start)
            self.sent[(piece, tag, digit, way)] = (block, exists, own)

    def events(self, piece):
        order = self.pieces[piece][0]
        here = {d: place(d) for d in order}
        found = []

        def begin(after):
            for digit in order:
                self.send(piece, here, None, digit, None, (), own=True)

        found.append((0, begin, ()))

        def arrivals(stage, block, exists, tag, depth):
            digit = order[stage]
            for hop, travel, q, there in relatives(digit):
                source = {**block, digit: q}
                condition = both(exists, there)
                label = tag + ((digit, hop, travel),)

                def arrive(after, source=source, condition=condition, travel=travel, label=label):
                    offset, _ = moves(digit)[0]
                    when(condition, self.copy(piece, source, digit, offset, 0, False).wait_recv)
                    if digit[2] > 2:
                        self.send(piece, source, condition, digit, (0 if travel > 0 else 1,), label)
                    for later in order[stage + 1 :]:
                        self.send(piece, source, condition, later, None, label)
                    if after is not None:
                        after(piece, source, condition, label)

                found.append((depth + hop, arrive, label))

        def expand(stage, earlier, block, exists, tag, depth):
            if earlier == stage:
                arrivals(stage, block, exists, tag, depth)
                return
            digit = order[earlier]
            expand(stage, earlier + 1, {**block, digit: here[digit]}, exists, tag, depth)
            for hop, travel, q, there in relatives(digit):
                expand(
                    stage, earlier + 1, {**block, digit: q}, both(exists, there),
                    tag + ((digit, hop, travel),), depth + hop,
                )

        for stage in range(len(order)):
            expand(stage, 0, dict(here), None, (), 0)
        return found

    def queue(self):
        entries = []
        for piece in range(len(self.pieces)):
            for depth, action, tag in self.events(piece):
                entries.append((depth, piece, len(entries), action, tag))
        entries.sort(key=lambda entry: entry[:3])
        return [(piece, action, tag) for _, piece, _, action, tag in entries]

    def run(self, after=None):
        for _, action, _ in self.queue():
            action(after)

    def drain(self):
        for (piece, _, digit, way), (block, exists, own) in self.sent.items():
            offset, has = moves(digit)[way]
            copy = self.copy(piece, block, digit, offset, way, own)
            when(both(exists, has), copy.wait_send)


def gather_kernel(layout, pieces, x_ref, out_ref, send_sem, recv_sem, local_sem):
    barrier_all(layout)
    gather = Gather(layout, pieces, out_ref, x_ref, send_sem, recv_sem)
    gather.run()
    local = pltpu.make_async_copy(x_ref, out_ref.at[tuple(place(d) for d in layout)], local_sem)
    local.start()
    local.wait()
    gather.drain()


def pieces_of(rows, orders, chunks):
    units = max(1, rows // 16)
    chunks = min(chunks, units)
    cuts = [units * i // chunks * 16 for i in range(chunks)] + [rows]
    return [(orders[i % len(orders)], cuts[i], cuts[i + 1] - cuts[i]) for i in range(chunks)]


def events_of(order):
    total, held = 0, 1
    for digit in order:
        around = 1 if digit[2] == 2 else 2 * (digit[2] - 1)
        total += held * around
        held *= 1 + around
    return total


def gather(x, axes, layout, orders, chunks, ident, name):
    rows, columns = x.shape
    if rows % 16 or len(orders) * events_of(orders[0]) > 256:
        return lax.all_gather(x, axes, axis=0, tiled=True)
    pieces = pieces_of(rows, orders, chunks)
    dims = tuple(d[2] for d in layout)
    out = pl.pallas_call(
        functools.partial(gather_kernel, layout, pieces),
        out_shape=jax.ShapeDtypeStruct(dims + (rows, columns), x.dtype),
        in_specs=[pl.BlockSpec(memory_space=pltpu.VMEM)],
        out_specs=pl.BlockSpec(memory_space=pl.ANY),
        scratch_shapes=Gather.semaphores(layout, pieces) + [pltpu.SemaphoreType.DMA],
        compiler_params=pltpu.CompilerParams(collective_id=ident, has_side_effects=True),
        name=name,
    )(x)
    return out.reshape(math.prod(dims) * rows, columns)


def nt_dot(left, right):
    return lax.dot_general(
        left, right, (((1,), (1,)), ((), ())), preferred_element_type=jnp.float32
    )


def window_of(blocks):
    return blocks // 2 + 1


def gram_kernel(block, where_ref, x_ref, part_ref):
    blocks = x_ref.shape[0] // block
    mine = part_ref.shape[0] // block
    window = part_ref.shape[1] // block
    first = where_ref[0] * mine
    left_at = pl.ds(pl.multiple_of(first * block, block), mine * block)
    for j in range(mine + window - 1):
        low, high = max(0, j - window + 1), min(mine - 1, j)
        other = lax.rem(first + j, blocks)
        right = x_ref[pl.ds(pl.multiple_of(other * block, block), block), :]
        rows = pl.ds(
            pl.multiple_of((first + low) * block, block), (high - low + 1) * block
        )
        product = nt_dot(x_ref[rows, :], right).astype(jnp.bfloat16)
        for i in range(low, high + 1):
            at = (i - low) * block
            part_ref[i * block : (i + 1) * block, (j - i) * block : (j - i + 1) * block] = (
                product[at : at + block, :]
            )


def reduce_kernel(
    block, rows, pieces, far, near, x_ref, columns_ref, share_ref, held, part, got_near, half, got_far,
    send_sem, recv_sem, near_send, near_recv, far_send, far_recv, out_sem,
):
    order = pieces[0][0]
    layout = tuple(sorted(order, key=lambda d: -d[1]))
    shards = math.prod(d[2] for d in layout)
    mine = x_ref.shape[0] // block
    window = part.shape[0]
    lines = far[2]
    axis = layout[0][0]
    shard = lax.axis_index(axis)
    barrier_lines(layout + (far, near))
    gather = Gather(layout, pieces, held, x_ref, send_sem, recv_sem)
    queue = gather.queue()
    starts = [entry for entry in queue if not entry[2]]
    events = [entry for entry in queue if entry[2]]

    def home(t, tag):
        for digit, _, _ in tag:
            _, stride, _, _ = digit
            t = t - stride if (t // stride) % 2 else t + stride
        return t

    def needed(t, d):
        wanted = set()
        for i in range(mine):
            s, piece = (i + d) // mine % shards, (i + d) % mine
            if s:
                wanted.add(((t + s) % shards, piece))
        return wanted

    slots = [[] for _ in range(window + 1)]
    done = [0] * shards
    for d in range(window + 1):
        begun = {}
        for t in range(shards):
            last = len(events)
            if d < window:
                wanted = needed(t, d)
                last = max(
                    [done[t]]
                    + [e + 1 for e, (piece, _, tag) in enumerate(events) if (home(t, tag), piece) in wanted]
                )
            for e in range(done[t], last):
                begun.setdefault(e, []).append(t)
            done[t] = last
        slots[d] = sorted(begun.items())

    copies = {}

    def keep(piece, source, condition, tag):
        _, row, count = pieces[piece]
        at = tuple(source[d] for d in layout) + (pl.ds(row, count), slice(None))
        number = next(e for e, entry in enumerate(events) if entry[0] == piece and entry[2] == tag)
        copies[number] = at
        pltpu.make_async_copy(held.at[at], columns_ref.at[at], out_sem.at[number]).start()

    for _, action, _ in starts:
        action(None)
    own = pltpu.make_async_copy(
        x_ref, columns_ref.at[tuple(place(d) for d in layout)], out_sem.at[len(events)]
    )
    own.start()

    def advance(d):
        for e, who in slots[d]:
            _, action, _ = events[e]
            if len(who) == shards:
                action(keep)
            else:
                condition = functools.reduce(lambda a, b: a | b, [shard == t for t in who])
                pl.when(condition)(functools.partial(action, keep))

    def owner_rows(far_place, near_place):
        start = (far_place * far[1] + near_place * near[1]) * rows
        return pl.ds(pl.multiple_of(start, 16), rows)

    def near_copy(d, line):
        return pltpu.make_async_remote_copy(
            src_ref=part.at[d, owner_rows(line, 1 - place(near)), :],
            dst_ref=got_near.at[d, line],
            send_sem=near_send.at[d, line],
            recv_sem=near_recv.at[d, line],
            device_id=peer(near, 1 - 2 * place(near)),
            device_id_type=pl.DeviceIdType.MESH,
        )

    def far_copy(d, step, arriving):
        there, offset = around(far, step)
        slot = there if arriving else place(far)
        return pltpu.make_async_remote_copy(
            src_ref=half.at[d, there],
            dst_ref=got_far.at[d, slot],
            send_sem=far_send.at[d, there],
            recv_sem=far_recv.at[d, slot],
            device_id=peer(far, offset),
            device_id_type=pl.DeviceIdType.MESH,
        )

    def form(d):
        for i in range(mine):
            s, piece = (i + d) // mine % shards, (i + d) % mine
            at = (pl.ds(piece * block, block), slice(None))
            if s:
                other = lax.rem(shard + s, shards)
                at = tuple(lax.rem(lax.div(other, g[1]), g[2]) for g in layout) + at
                right = held[at]
            else:
                right = x_ref[at]
            left = x_ref[i * block : (i + 1) * block, :]
            part[d, i * block : (i + 1) * block, :] = nt_dot(left, right).astype(jnp.bfloat16)
        for line in range(lines):
            near_copy(d, line).start()

    def halve(d):
        for line in range(lines):
            near_copy(d, line).wait_recv()
            half[d, line] = (
                part[d, owner_rows(line, place(near)), :].astype(jnp.float32)
                + got_near[d, line].astype(jnp.float32)
            ).astype(jnp.bfloat16)
        for step in range(1, lines):
            far_copy(d, step, False).start()

    def finish(d):
        total = half[d, place(far)].astype(jnp.float32)
        for step in range(1, lines):
            there, _ = around(far, step)
            far_copy(d, step, True).wait_recv()
            total = total + got_far[d, there].astype(jnp.float32)
        share_ref[:, d * block : (d + 1) * block] = total.astype(jnp.bfloat16)

    for d in range(window + 2):
        if d <= window:
            if d > 0:
                halve(d - 1)
            if d > 1:
                finish(d - 2)
            advance(d)
        else:
            finish(d - 2)
        if d < window:
            form(d)

    for d in range(window):
        for line in range(lines):
            near_copy(d, line).wait_send()
        for step in range(1, lines):
            far_copy(d, step, False).wait_send()
    for number, at in copies.items():
        pltpu.make_async_copy(held.at[at], columns_ref.at[at], out_sem.at[number]).wait()
    own.wait()
    gather.drain()


def reduced_gram(iterate, digits, block, window, ident):
    layout = tuple(digits["tp"])
    if len(digits["mats"]) != 2 or any(d[2] != 2 for d in layout):
        return None
    far, near = digits["mats"]
    mine, width = iterate.shape
    rows = mine // (far[2] * near[2])
    if near[2] != 2 or rows % 16 or mine % block:
        return None
    order = tuple(sorted(layout, key=lambda d: d[3]))
    pieces = [(order, row, block) for row in range(0, mine, block)]
    dims = tuple(d[2] for d in layout)
    chunks, lines = window // block, far[2]
    tile = pltpu.VMEM((chunks, lines, rows, block), jnp.bfloat16)
    dma = pltpu.SemaphoreType.DMA
    blocks = math.prod(dims) - 1
    columns, share = pl.pallas_call(
        functools.partial(reduce_kernel, block, rows, pieces, far, near),
        out_shape=(
            jax.ShapeDtypeStruct(dims + iterate.shape, jnp.bfloat16),
            jax.ShapeDtypeStruct((rows, window), jnp.bfloat16),
        ),
        in_specs=[pl.BlockSpec(memory_space=pltpu.VMEM)],
        out_specs=(pl.BlockSpec(memory_space=pl.ANY), pl.BlockSpec(memory_space=pltpu.VMEM)),
        scratch_shapes=[
            pltpu.VMEM(dims + iterate.shape, jnp.bfloat16),
            pltpu.VMEM((chunks, mine, block), jnp.bfloat16),
            tile, tile, tile,
        ]
        + Gather.semaphores(layout, pieces)
        + [dma((chunks, lines))] * 4
        + [dma((blocks * len(pieces) + 1,))],
        compiler_params=pltpu.CompilerParams(
            collective_id=ident, has_side_effects=True, vmem_limit_bytes=grant
        ),
        name="reduced_gram",
    )(iterate)
    return columns.reshape(dims[0] * math.prod(dims[1:]) * mine, width), share


def poly_kernel(block, scale, where_ref, compact_ref, out_ref, kappa_ref, gram, own, one, two, left, right):
    size = gram.shape[0]
    blocks = size // block
    window = compact_ref.shape[1] // block
    for i in range(blocks):
        for d in range(window):
            j = (i + d) % blocks
            tile = compact_ref[i * block : (i + 1) * block, d * block : (d + 1) * block]
            gram[i * block : (i + 1) * block, j * block : (j + 1) * block] = tile
            if d > 0 and 2 * d != blocks:
                gram[j * block : (j + 1) * block, i * block : (i + 1) * block] = tile.T

    def column_sums(step, total):
        rows = jnp.abs(gram[pl.ds(pl.multiple_of(step * 16, 16), 16), :].astype(jnp.float32))
        return total + (rows[0:8] + rows[8:16])

    total = lax.fori_loop(0, size // 16, column_sums, jnp.zeros((8, size), jnp.float32))
    bound = jnp.max(jnp.sum(total, axis=0, keepdims=True), axis=1, keepdims=True) + epsilon
    root = lax.rsqrt(jnp.broadcast_to(bound, (1, 128)))
    kappa = (scale * first_coef * first_coef) * root
    kappa_ref[...] = kappa
    inverse = (root * root)[:, :1]
    count = own.shape[0]
    width = math.gcd(size, 1024)

    def columns(body):
        @pl.loop(0, size // width)
        def _(step):
            body(pl.ds(pl.multiple_of(step * width, width), width))

    def times_gram(source, at):
        return inverse * jnp.dot(source[...], gram[:, at], preferred_element_type=jnp.float32)

    def wide(ref, at):
        return ref[:, at].astype(jnp.float32)

    def apply(source, target, constant=None):
        def body(at):
            value = times_gram(source, at)
            if constant is not None:
                value = value + (constant * inverse) * wide(own, at)
            target[:, at] = value.astype(jnp.bfloat16)

        columns(body)

    def polynomial(source, middle, target):
        apply(source, middle)

        def body(at):
            target[:, at] = (
                first_coef * wide(source, at)
                + second_coef * wide(middle, at)
                + third_coef * times_gram(middle, at)
            ).astype(jnp.bfloat16)

        columns(body)

    if count % 16 == 0:
        own[...] = gram[pl.ds(pl.multiple_of(where_ref[0] * count, 16), count), :]
    else:
        row = lax.broadcasted_iota(jnp.int32, (count, size), 0) + where_ref[0] * count
        column = lax.broadcasted_iota(jnp.int32, (count, size), 1)
        two[...] = (row == column).astype(jnp.float32).astype(jnp.bfloat16)

        def select(at):
            own[:, at] = jnp.dot(
                two[...], gram[:, at], preferred_element_type=jnp.float32
            ).astype(jnp.bfloat16)

        columns(select)

    def start(at):
        left[:, at] = (inverse * wide(own, at)).astype(jnp.bfloat16)

    columns(start)

    def first(at):
        one[:, at] = (
            second_coef * wide(left, at) + third_coef * times_gram(left, at)
        ).astype(jnp.bfloat16)

    columns(first)
    apply(one, left, first_coef)
    polynomial(left, right, two)
    polynomial(two, right, left)

    def keep(at):
        two[:, at] = left[:, at]

    columns(keep)
    apply(two, right)
    polynomial(right, left, own)
    polynomial(own, left, right)

    def finish(at):
        mixed = (
            first_coef * wide(one, at) + second_coef * wide(two, at) + third_coef * wide(right, at)
        )
        out_ref[:, at] = ((scale * root[:, :1]) * mixed).astype(jnp.bfloat16)

    columns(finish)


def orders_of(digits):
    layout = tuple(digits["tp"]) + tuple(digits["mats"])
    far = {axis: [d for d in found if not d[3]] for axis, found in digits.items()}
    near = [d for d in layout if d[3]]
    one = tuple(far["mats"] + far["tp"] + near)
    two = tuple(far["mats"][:1] + far["tp"] + far["mats"][1:] + near)
    return layout, [one, two] if one != two else [one]


def per_device(scale, digits, grad, momentum):
    new_momentum = momentum_beta * momentum + grad.astype(jnp.float32)
    iterate = (grad.astype(jnp.float32) + momentum_beta * new_momentum).astype(jnp.bfloat16)
    layout, orders = orders_of(digits)
    lines = {axis: tuple(sorted(found, key=lambda d: d[3])) for axis, found in digits.items()}
    size = momentum.shape[0] * lax.axis_size("tp")
    mine = iterate.shape[0]
    block = math.gcd(mine, 256)
    window = window_of(size // block) * block
    smem = pl.BlockSpec(memory_space=pltpu.SMEM)
    whole = pl.BlockSpec(memory_space=pltpu.VMEM)
    params = pltpu.CompilerParams(vmem_limit_bytes=grant)
    tp = lax.axis_index("tp")
    fused = reduced_gram(iterate, digits, block, window, 1)
    if fused is not None:
        columns, share = fused
    else:
        columns = gather(iterate, "tp", tuple(digits["tp"]), [lines["tp"]], 6, 1, "gather_x")
        part = pl.pallas_call(
            functools.partial(gram_kernel, block),
            out_shape=jax.ShapeDtypeStruct((mine, window), jnp.bfloat16),
            in_specs=[smem, whole],
            out_specs=whole,
            compiler_params=params,
            name="gram",
        )(tp.reshape(1), columns)
        share = lax.psum_scatter(part, "mats", scatter_dimension=0, tiled=True)
    compact = gather(share, ("tp", "mats"), layout, orders, 2, 2, "gather_gram")
    count = share.shape[0]
    place = tp * lax.axis_size("mats") + lax.axis_index("mats")
    thin = pltpu.VMEM((count, size), jnp.bfloat16)
    rows, kappa = pl.pallas_call(
        functools.partial(poly_kernel, block, scale),
        out_shape=(
            jax.ShapeDtypeStruct((count, size), jnp.bfloat16),
            jax.ShapeDtypeStruct((1, 128), jnp.float32),
        ),
        in_specs=[smem, whole],
        out_specs=(whole, whole),
        scratch_shapes=[pltpu.VMEM((size, size), jnp.bfloat16)] + [thin] * 5,
        compiler_params=params,
        cost_estimate=pl.CostEstimate(
            flops=22 * count * size * size, bytes_accessed=size * window * 2, transcendentals=0
        ),
        name="poly",
    )(place.reshape(1), compact)
    matrix = gather(rows, "mats", tuple(digits["mats"]), [lines["mats"]], 3, 3, "gather_rows")
    product = jnp.dot(matrix, columns, preferred_element_type=jnp.float32)
    update = (product + kappa[0, 0] * iterate.astype(jnp.float32)).astype(jnp.bfloat16)
    return (update, new_momentum)


def solution(mesh):
    digits = digits_of(mesh)

    def step(grad, momentum):
        scale = shape_gain * math.sqrt(max(grad.shape))
        return jax.shard_map(
            functools.partial(per_device, scale, digits),
            mesh=mesh,
            in_specs=(P("tp", "mats"), P("tp", "mats")),
            out_specs=(P("tp", "mats"), P("tp", "mats")),
            check_vma=False,
        )(grad, momentum)

    return step
```

```python
import functools
import math

import jax
import jax.numpy as jnp
from jax import lax
from jax.experimental import pallas as pl
from jax.experimental.pallas import tpu as pltpu
from jax.sharding import PartitionSpec as P

momentum_beta = 0.95
first_coef = 3.4445
second_coef = -4.775
third_coef = 2.0315
shape_gain = 0.2
epsilon = 1e-06
grant = 62 * 1024 * 1024


def digits_of(mesh):
    table = {}
    shape = mesh.devices.shape
    for number, axis in enumerate(mesh.axis_names):
        extent = shape[number]
        line = [mesh.devices[tuple(i if k == number else 0 for k in range(len(shape)))] for i in range(extent)]
        found = []
        if all(hasattr(device, "coords") for device in line):
            places = [(*device.coords, device.core_on_chip) for device in line]
            for place, column in enumerate(zip(*places)):
                kinds = len(set(column))
                if kinds > 1:
                    stride = next(i for i in range(extent) if column[i] != column[0])
                    if all((i // stride) % kinds == column[i] - column[0] for i in range(extent)):
                        found.append((axis, stride, kinds, place == 3))
        if math.prod(kinds for _, _, kinds, _ in found) != extent:
            found = [(axis, 1, extent, False)]
        table[axis] = sorted(found, key=lambda digit: -digit[1])
    return table


def place(digit):
    axis, stride, extent, _ = digit
    return lax.rem(lax.div(lax.axis_index(axis), stride), extent)


def moves(digit):
    here, extent = place(digit), digit[2]
    if extent == 2:
        return [(1 - 2 * here, None)]
    return [(1, here + 1 < extent), (-1, here >= 1)]


def when(condition, body):
    if condition is None:
        body()
    else:
        pl.when(condition)(body)


def both(*conditions):
    found = [c for c in conditions if c is not None]
    return functools.reduce(lambda a, b: a & b, found) if found else None


def peer(digit, offset):
    axis, stride, _, _ = digit
    return {axis: lax.axis_index(axis) + offset * stride}


def barrier_all(digits):
    semaphore = pltpu.get_barrier_semaphore()
    for digit in digits:
        for offset, has in moves(digit):
            when(has, functools.partial(
                pl.semaphore_signal, semaphore, inc=1, device_id=peer(digit, offset),
                device_id_type=pl.DeviceIdType.MESH))
    count = 0
    for digit in digits:
        for _, has in moves(digit):
            count = count + (1 if has is None else has.astype(jnp.int32))
    pl.semaphore_wait(semaphore, count)


def around(digit, step):
    here = place(digit)
    there = lax.rem(here + step, digit[2])
    return there, there - here


def barrier_lines(digits):
    semaphore = pltpu.get_barrier_semaphore()
    count = 0
    for digit in digits:
        for step in range(1, digit[2]):
            _, offset = around(digit, step)
            pl.semaphore_signal(
                semaphore, inc=1, device_id=peer(digit, offset),
                device_id_type=pl.DeviceIdType.MESH,
            )
            count += 1
    pl.semaphore_wait(semaphore, count)


def relatives(digit):
    here, extent = place(digit), digit[2]
    if extent == 2:
        return [(1, 0, 1 - here, None)]
    found = []
    for hop in range(1, extent):
        found.append((hop, 1, here - hop, here >= hop))
        found.append((hop, -1, here + hop, here + hop < extent))
    return found


class Gather:
    def __init__(self, layout, pieces, buffer, source, send_sem, recv_sem):
        self.layout, self.pieces, self.buffer, self.source = layout, pieces, buffer, source
        self.send_sem, self.recv_sem = send_sem, recv_sem
        self.sent = {}

    @staticmethod
    def semaphores(layout, pieces):
        dims = tuple(d[2] for d in layout)
        return [
            pltpu.SemaphoreType.DMA((len(pieces), 2 * len(layout)) + dims),
            pltpu.SemaphoreType.DMA((len(pieces),) + dims),
        ]

    def copy(self, piece, block, digit, offset, way, own):
        order, row, count = self.pieces[piece]
        index = tuple(block[d] for d in self.layout)
        rows = (pl.ds(row, count), slice(None))
        at = self.buffer.at[index + rows]
        lane = 2 * self.layout.index(digit) + way
        return pltpu.make_async_remote_copy(
            src_ref=self.source.at[rows] if own else at,
            dst_ref=at,
            send_sem=self.send_sem.at[(piece, lane) + index],
            recv_sem=self.recv_sem.at[(piece,) + index],
            device_id=peer(digit, offset),
            device_id_type=pl.DeviceIdType.MESH,
        )

    def send(self, piece, block, exists, digit, directions, tag, own=False):
        for way, (offset, has) in enumerate(moves(digit)):
            if directions is not None and way not in directions:
                continue
            copy = self.copy(piece, block, digit, offset, way, own)
            condition = both(exists, has)
            when(condition, copy.start)
            self.sent[(piece, tag, digit, way)] = (block, exists, own)

    def events(self, piece):
        order = self.pieces[piece][0]
        here = {d: place(d) for d in order}
        found = []

        def begin(after):
            for digit in order:
                self.send(piece, here, None, digit, None, (), own=True)

        found.append((0, begin, ()))

        def arrivals(stage, block, exists, tag, depth):
            digit = order[stage]
            for hop, travel, q, there in relatives(digit):
                source = {**block, digit: q}
                condition = both(exists, there)
                label = tag + ((digit, hop, travel),)

                def arrive(after, source=source, condition=condition, travel=travel, label=label):
                    offset, _ = moves(digit)[0]
                    when(condition, self.copy(piece, source, digit, offset, 0, False).wait_recv)
                    if digit[2] > 2:
                        self.send(piece, source, condition, digit, (0 if travel > 0 else 1,), label)
                    for later in order[stage + 1 :]:
                        self.send(piece, source, condition, later, None, label)
                    if after is not None:
                        after(piece, source, condition, label)

                found.append((depth + hop, arrive, label))

        def expand(stage, earlier, block, exists, tag, depth):
            if earlier == stage:
                arrivals(stage, block, exists, tag, depth)
                return
            digit = order[earlier]
            expand(stage, earlier + 1, {**block, digit: here[digit]}, exists, tag, depth)
            for hop, travel, q, there in relatives(digit):
                expand(
                    stage, earlier + 1, {**block, digit: q}, both(exists, there),
                    tag + ((digit, hop, travel),), depth + hop,
                )

        for stage in range(len(order)):
            expand(stage, 0, dict(here), None, (), 0)
        return found

    def queue(self):
        entries = []
        for piece in range(len(self.pieces)):
            for depth, action, tag in self.events(piece):
                entries.append((depth, piece, len(entries), action, tag))
        entries.sort(key=lambda entry: entry[:3])
        return [(piece, action, tag) for _, piece, _, action, tag in entries]

    def run(self, after=None):
        for _, action, _ in self.queue():
            action(after)

    def drain(self):
        for (piece, _, digit, way), (block, exists, own) in self.sent.items():
            offset, has = moves(digit)[way]
            copy = self.copy(piece, block, digit, offset, way, own)
            when(both(exists, has), copy.wait_send)


def gather_kernel(layout, pieces, x_ref, out_ref, send_sem, recv_sem, local_sem):
    barrier_all(layout)
    gather = Gather(layout, pieces, out_ref, x_ref, send_sem, recv_sem)
    gather.run()
    local = pltpu.make_async_copy(x_ref, out_ref.at[tuple(place(d) for d in layout)], local_sem)
    local.start()
    local.wait()
    gather.drain()


def pieces_of(rows, orders, chunks):
    units = max(1, rows // 16)
    chunks = min(chunks, units)
    cuts = [units * i // chunks * 16 for i in range(chunks)] + [rows]
    return [(orders[i % len(orders)], cuts[i], cuts[i + 1] - cuts[i]) for i in range(chunks)]


def events_of(order):
    total, held = 0, 1
    for digit in order:
        around = 1 if digit[2] == 2 else 2 * (digit[2] - 1)
        total += held * around
        held *= 1 + around
    return total


def gather(x, axes, layout, orders, chunks, ident, name):
    rows, columns = x.shape
    if rows % 16 or len(orders) * events_of(orders[0]) > 256:
        return lax.all_gather(x, axes, axis=0, tiled=True)
    pieces = pieces_of(rows, orders, chunks)
    dims = tuple(d[2] for d in layout)
    out = pl.pallas_call(
        functools.partial(gather_kernel, layout, pieces),
        out_shape=jax.ShapeDtypeStruct(dims + (rows, columns), x.dtype),
        in_specs=[pl.BlockSpec(memory_space=pltpu.VMEM)],
        out_specs=pl.BlockSpec(memory_space=pl.ANY),
        scratch_shapes=Gather.semaphores(layout, pieces) + [pltpu.SemaphoreType.DMA],
        compiler_params=pltpu.CompilerParams(collective_id=ident, has_side_effects=True),
        name=name,
    )(x)
    return out.reshape(math.prod(dims) * rows, columns)


def nt_dot(left, right):
    return lax.dot_general(
        left, right, (((1,), (1,)), ((), ())), preferred_element_type=jnp.float32
    )


def window_of(blocks):
    return blocks // 2 + 1


def gram_kernel(block, where_ref, x_ref, part_ref):
    blocks = x_ref.shape[0] // block
    mine = part_ref.shape[0] // block
    window = part_ref.shape[1] // block
    first = where_ref[0] * mine
    left_at = pl.ds(pl.multiple_of(first * block, block), mine * block)
    for j in range(mine + window - 1):
        low, high = max(0, j - window + 1), min(mine - 1, j)
        other = lax.rem(first + j, blocks)
        right = x_ref[pl.ds(pl.multiple_of(other * block, block), block), :]
        rows = pl.ds(
            pl.multiple_of((first + low) * block, block), (high - low + 1) * block
        )
        product = nt_dot(x_ref[rows, :], right).astype(jnp.bfloat16)
        for i in range(low, high + 1):
            at = (i - low) * block
            part_ref[i * block : (i + 1) * block, (j - i) * block : (j - i + 1) * block] = (
                product[at : at + block, :]
            )


def reduce_kernel(
    block, rows, pieces, far, near, x_ref, columns_ref, share_ref, held, part, got_near, half, got_far,
    send_sem, recv_sem, near_send, near_recv, far_send, far_recv, out_sem,
):
    order = pieces[0][0]
    layout = tuple(sorted(order, key=lambda d: -d[1]))
    shards = math.prod(d[2] for d in layout)
    mine = x_ref.shape[0] // block
    window = part.shape[0]
    lines = far[2]
    axis = layout[0][0]
    shard = lax.axis_index(axis)
    barrier_lines(layout + (far, near))
    gather = Gather(layout, pieces, held, x_ref, send_sem, recv_sem)
    queue = gather.queue()
    starts = [entry for entry in queue if not entry[2]]
    events = [entry for entry in queue if entry[2]]

    def home(t, tag):
        for digit, _, _ in tag:
            _, stride, _, _ = digit
            t = t - stride if (t // stride) % 2 else t + stride
        return t

    def needed(t, d):
        wanted = set()
        for i in range(mine):
            s, piece = (i + d) // mine % shards, (i + d) % mine
            if s:
                wanted.add(((t + s) % shards, piece))
        return wanted

    slots = [[] for _ in range(window + 1)]
    done = [0] * shards
    for d in range(window + 1):
        begun = {}
        for t in range(shards):
            last = len(events)
            if d < window:
                wanted = needed(t, d)
                last = max(
                    [done[t]]
                    + [e + 1 for e, (piece, _, tag) in enumerate(events) if (home(t, tag), piece) in wanted]
                )
            for e in range(done[t], last):
                begun.setdefault(e, []).append(t)
            done[t] = last
        slots[d] = sorted(begun.items())

    copies = {}

    def keep(piece, source, condition, tag):
        _, row, count = pieces[piece]
        at = tuple(source[d] for d in layout) + (pl.ds(row, count), slice(None))
        number = next(e for e, entry in enumerate(events) if entry[0] == piece and entry[2] == tag)
        copies[number] = at
        pltpu.make_async_copy(held.at[at], columns_ref.at[at], out_sem.at[number]).start()

    for _, action, _ in starts:
        action(None)
    own = pltpu.make_async_copy(
        x_ref, columns_ref.at[tuple(place(d) for d in layout)], out_sem.at[len(events)]
    )
    own.start()

    def advance(d):
        for e, who in slots[d]:
            _, action, _ = events[e]
            if len(who) == shards:
                action(keep)
            else:
                condition = functools.reduce(lambda a, b: a | b, [shard == t for t in who])
                pl.when(condition)(functools.partial(action, keep))

    def owner_rows(far_place, near_place):
        start = (far_place * far[1] + near_place * near[1]) * rows
        return pl.ds(pl.multiple_of(start, 16), rows)

    def near_copy(d, line):
        return pltpu.make_async_remote_copy(
            src_ref=part.at[d, owner_rows(line, 1 - place(near)), :],
            dst_ref=got_near.at[d, line],
            send_sem=near_send.at[d, line],
            recv_sem=near_recv.at[d, line],
            device_id=peer(near, 1 - 2 * place(near)),
            device_id_type=pl.DeviceIdType.MESH,
        )

    def far_copy(d, step, arriving):
        there, offset = around(far, step)
        slot = there if arriving else place(far)
        return pltpu.make_async_remote_copy(
            src_ref=half.at[d, there],
            dst_ref=got_far.at[d, slot],
            send_sem=far_send.at[d, there],
            recv_sem=far_recv.at[d, slot],
            device_id=peer(far, offset),
            device_id_type=pl.DeviceIdType.MESH,
        )

    def form(d):
        for i in range(mine):
            s, piece = (i + d) // mine % shards, (i + d) % mine
            at = (pl.ds(piece * block, block), slice(None))
            if s:
                other = lax.rem(shard + s, shards)
                at = tuple(lax.rem(lax.div(other, g[1]), g[2]) for g in layout) + at
                right = held[at]
            else:
                right = x_ref[at]
            left = x_ref[i * block : (i + 1) * block, :]
            part[d, i * block : (i + 1) * block, :] = nt_dot(left, right).astype(jnp.bfloat16)
        for line in range(lines):
            near_copy(d, line).start()

    def halve(d):
        for line in range(lines):
            near_copy(d, line).wait_recv()
            half[d, line] = (
                part[d, owner_rows(line, place(near)), :].astype(jnp.float32)
                + got_near[d, line].astype(jnp.float32)
            ).astype(jnp.bfloat16)
        for step in range(1, lines):
            far_copy(d, step, False).start()

    def finish(d):
        total = half[d, place(far)].astype(jnp.float32)
        for step in range(1, lines):
            there, _ = around(far, step)
            far_copy(d, step, True).wait_recv()
            total = total + got_far[d, there].astype(jnp.float32)
        share_ref[:, d * block : (d + 1) * block] = total.astype(jnp.bfloat16)

    for d in range(window + 2):
        if d <= window:
            if d > 0:
                halve(d - 1)
            if d > 1:
                finish(d - 2)
            advance(d)
        else:
            finish(d - 2)
        if d < window:
            form(d)

    for d in range(window):
        for line in range(lines):
            near_copy(d, line).wait_send()
        for step in range(1, lines):
            far_copy(d, step, False).wait_send()
    for number, at in copies.items():
        pltpu.make_async_copy(held.at[at], columns_ref.at[at], out_sem.at[number]).wait()
    own.wait()
    gather.drain()


def reduced_gram(iterate, digits, block, window, ident):
    layout = tuple(digits["tp"])
    if len(digits["mats"]) != 2 or any(d[2] != 2 for d in layout):
        return None
    far, near = digits["mats"]
    mine, width = iterate.shape
    rows = mine // (far[2] * near[2])
    if near[2] != 2 or rows % 16 or mine % block:
        return None
    order = tuple(sorted(layout, key=lambda d: d[3]))
    pieces = [(order, row, block) for row in range(0, mine, block)]
    dims = tuple(d[2] for d in layout)
    chunks, lines = window // block, far[2]
    tile = pltpu.VMEM((chunks, lines, rows, block), jnp.bfloat16)
    dma = pltpu.SemaphoreType.DMA
    blocks = math.prod(dims) - 1
    columns, share = pl.pallas_call(
        functools.partial(reduce_kernel, block, rows, pieces, far, near),
        out_shape=(
            jax.ShapeDtypeStruct(dims + iterate.shape, jnp.bfloat16),
            jax.ShapeDtypeStruct((rows, window), jnp.bfloat16),
        ),
        in_specs=[pl.BlockSpec(memory_space=pltpu.VMEM)],
        out_specs=(pl.BlockSpec(memory_space=pl.ANY), pl.BlockSpec(memory_space=pltpu.VMEM)),
        scratch_shapes=[
            pltpu.VMEM(dims + iterate.shape, jnp.bfloat16),
            pltpu.VMEM((chunks, mine, block), jnp.bfloat16),
            tile, tile, tile,
        ]
        + Gather.semaphores(layout, pieces)
        + [dma((chunks, lines))] * 4
        + [dma((blocks * len(pieces) + 1,))],
        compiler_params=pltpu.CompilerParams(
            collective_id=ident, has_side_effects=True, vmem_limit_bytes=grant
        ),
        name="reduced_gram",
    )(iterate)
    return columns.reshape(dims[0] * math.prod(dims[1:]) * mine, width), share


def polynomial_rows(gram, own, one, two, left, right, scale, where_ref):
    size = gram.shape[0]

    def column_sums(step, total):
        rows = jnp.abs(gram[pl.ds(pl.multiple_of(step * 16, 16), 16), :].astype(jnp.float32))
        return total + (rows[0:8] + rows[8:16])

    total = lax.fori_loop(0, size // 16, column_sums, jnp.zeros((8, size), jnp.float32))
    bound = jnp.max(jnp.sum(total, axis=0, keepdims=True), axis=1, keepdims=True) + epsilon
    root = lax.rsqrt(jnp.broadcast_to(bound, (1, 128)))
    inverse = (root * root)[:, :1]
    count = own.shape[0]
    width = math.gcd(size, 1024)
    if where_ref is None:
        index = lax.axis_index("tp") * lax.axis_size("mats") + lax.axis_index("mats")
    else:
        index = where_ref[0]

    def columns(body):
        @pl.loop(0, size // width)
        def _(step):
            body(pl.ds(pl.multiple_of(step * width, width), width))

    def times_gram(source, at):
        return inverse * jnp.dot(source[...], gram[:, at], preferred_element_type=jnp.float32)

    def wide(ref, at):
        return ref[:, at].astype(jnp.float32)

    def apply(source, target, constant=None):
        def body(at):
            value = times_gram(source, at)
            if constant is not None:
                value = value + (constant * inverse) * wide(own, at)
            target[:, at] = value.astype(jnp.bfloat16)

        columns(body)

    def polynomial(source, middle, target):
        apply(source, middle)

        def body(at):
            target[:, at] = (
                first_coef * wide(source, at)
                + second_coef * wide(middle, at)
                + third_coef * times_gram(middle, at)
            ).astype(jnp.bfloat16)

        columns(body)

    if count % 16 == 0:
        own[...] = gram[pl.ds(pl.multiple_of(index * count, 16), count), :]
    else:
        row = lax.broadcasted_iota(jnp.int32, (count, size), 0) + index * count
        column = lax.broadcasted_iota(jnp.int32, (count, size), 1)
        two[...] = (row == column).astype(jnp.float32).astype(jnp.bfloat16)

        def select(at):
            own[:, at] = jnp.dot(
                two[...], gram[:, at], preferred_element_type=jnp.float32
            ).astype(jnp.bfloat16)

        columns(select)

    def start(at):
        left[:, at] = (inverse * wide(own, at)).astype(jnp.bfloat16)

    columns(start)

    def first(at):
        one[:, at] = (
            second_coef * wide(left, at) + third_coef * times_gram(left, at)
        ).astype(jnp.bfloat16)

    columns(first)
    apply(one, left, first_coef)
    polynomial(left, right, two)
    polynomial(two, right, left)

    def keep(at):
        two[:, at] = left[:, at]

    columns(keep)
    apply(two, right)
    polynomial(right, left, own)
    polynomial(own, left, right)

    def finish(at):
        mixed = (
            first_coef * wide(one, at) + second_coef * wide(two, at) + third_coef * wide(right, at)
        )
        left[:, at] = ((scale * root[:, :1]) * mixed).astype(jnp.bfloat16)

    columns(finish)
    return root


def poly_kernel(block, scale, where_ref, compact_ref, out_ref, kappa_ref, gram, own, one, two, left, right):
    size = gram.shape[0]
    blocks = size // block
    window = compact_ref.shape[1] // block
    for i in range(blocks):
        for d in range(window):
            j = (i + d) % blocks
            tile = compact_ref[i * block : (i + 1) * block, d * block : (d + 1) * block]
            gram[i * block : (i + 1) * block, j * block : (j + 1) * block] = tile
            if d > 0 and 2 * d != blocks:
                gram[j * block : (j + 1) * block, i * block : (i + 1) * block] = tile.T

    root = polynomial_rows(gram, own, one, two, left, right, scale, where_ref)
    kappa_ref[...] = (scale * first_coef * first_coef) * root
    out_ref[...] = left[...]


def finish_kernel(
    block, scale, layout, pieces, near_pieces, share_ref, columns_ref, out_ref, held, gram, own, one, two, left,
    right, rows, columns, result, send_sem, recv_sem, rows_send, rows_recv, in_sem, out_sem,
):
    barrier_all(layout)
    tp = tuple(d for d in layout if d[0] == "tp")
    far, near = (d for d in layout if d[0] == "mats")
    load = pltpu.make_async_copy(columns_ref, columns, in_sem)
    gather = Gather(layout, pieces, held, share_ref, send_sem, recv_sem)
    queue = gather.queue()
    for _, action, tag in queue:
        if not tag:
            action(None)
    load.start()
    held[tuple(place(d) for d in layout)] = share_ref[...]
    for _, action, tag in queue:
        if tag:
            action(None)

    size = gram.shape[0]
    count, window = share_ref.shape
    blocks = size // block
    shards = math.prod(d[2] for d in tp)
    mine = size // shards
    for t in range(shards):
        at = tuple((t // d[1]) % d[2] for d in tp)
        for d in range(window // block):
            strip = held[at + (slice(None), slice(None), slice(None), pl.ds(d * block, block))]
            strip = strip.reshape(mine, block)
            for k in range(mine // block):
                i = t * (mine // block) + k
                j = (i + d) % blocks
                tile = strip[k * block : (k + 1) * block, :]
                gram[i * block : (i + 1) * block, j * block : (j + 1) * block] = tile
                if d > 0 and 2 * d != blocks:
                    gram[j * block : (j + 1) * block, i * block : (i + 1) * block] = tile.T

    root = polynomial_rows(gram, own, one, two, left, right, scale, None)
    kappa = ((scale * first_coef * first_coef) * root)[:, :1]

    spread = Gather((far, near), near_pieces, rows, left, rows_send, rows_recv)
    queue = spread.queue()
    for _, action, tag in queue:
        if not tag:
            action(None)
    rows[place(far), place(near)] = left[...]
    load.wait()
    pair = near[2] * count
    width = math.gcd(columns.shape[1], 512)
    shard_row = lax.axis_index("tp") * mine

    def multiply(line):
        matrix = rows[line].reshape(pair, size)
        at = pl.ds(pl.multiple_of(line * pair, 16), pair)
        mirror = pl.ds(pl.multiple_of(shard_row + line * pair, 16), pair)

        @pl.loop(0, columns.shape[1] // width)
        def _(step):
            across = pl.ds(pl.multiple_of(step * width, width), width)
            product = jnp.dot(matrix, columns[:, across], preferred_element_type=jnp.float32)
            result[at, across] = (
                product + kappa * columns[mirror, across].astype(jnp.float32)
            ).astype(jnp.bfloat16)

        pltpu.make_async_copy(result.at[at], out_ref.at[at], out_sem.at[line]).start()

    groups = [(None, place(far), None)]
    groups += [((far, hop, travel), q, there) for hop, travel, q, there in relatives(far)]
    missing = []
    for label, q, there in groups:
        wanted = set()
        for piece, _, tag in queue:
            if tag and [part for part in tag if part[0] == far] == ([label] if label else []):
                wanted.add((piece, tag))
        missing.append((wanted, q, there))
    for piece, action, tag in queue:
        if not tag:
            continue
        action(None)
        for wanted, q, there in missing:
            if (piece, tag) in wanted:
                wanted.remove((piece, tag))
                if not wanted:
                    when(there, functools.partial(multiply, q))
    for line in range(far[2]):
        at = pl.ds(line * pair, pair)
        pltpu.make_async_copy(result.at[at], out_ref.at[at], out_sem.at[line]).wait()
    gather.drain()
    spread.drain()


def finished(share, columns, digits, block, scale, ident):
    layout, _ = orders_of(digits)
    count, window = share.shape
    if len(digits["mats"]) != 2 or len(digits["tp"]) != 2 or digits["mats"][1][2] != 2 or count % 16:
        return None
    far, near = digits["mats"]
    side = [d for d in digits["tp"] if not d[3]]
    close = tuple(d for d in digits["tp"] if d[3])
    if len(side) != 1 or any(d[2] != 2 for d in digits["tp"]):
        return None
    orders = [(far, near, side[0]) + close, (far, side[0], near) + close]
    pieces = pieces_of(count, orders, 2)
    most = (count * 5 // 6 + 15) // 16 * 16
    near_pieces = [((far, near), 0, most)]
    if most < count:
        near_pieces.append(((near, far), most, count - most))
    size, width = columns.shape
    dims = tuple(d[2] for d in layout)
    mine = count * far[2] * near[2]
    thin = pltpu.VMEM((count, size), jnp.bfloat16)
    return pl.pallas_call(
        functools.partial(finish_kernel, block, scale, layout, pieces, near_pieces),
        out_shape=jax.ShapeDtypeStruct((mine, width), jnp.bfloat16),
        in_specs=[pl.BlockSpec(memory_space=pltpu.VMEM), pl.BlockSpec(memory_space=pl.ANY)],
        out_specs=pl.BlockSpec(memory_space=pl.ANY),
        scratch_shapes=[
            pltpu.VMEM(dims + share.shape, jnp.bfloat16),
            pltpu.VMEM((size, size), jnp.bfloat16),
        ]
        + [thin] * 5
        + [
            pltpu.VMEM((far[2], near[2], count, size), jnp.bfloat16),
            pltpu.VMEM((size, width), jnp.bfloat16),
            pltpu.VMEM((mine, width), jnp.bfloat16),
        ]
        + Gather.semaphores(layout, pieces)
        + Gather.semaphores((far, near), near_pieces)
        + [pltpu.SemaphoreType.DMA, pltpu.SemaphoreType.DMA((far[2],))],
        compiler_params=pltpu.CompilerParams(
            collective_id=ident, has_side_effects=True, vmem_limit_bytes=63 * 1024 * 1024
        ),
        name="finished",
    )(share, columns)


def orders_of(digits):
    layout = tuple(digits["tp"]) + tuple(digits["mats"])
    far = {axis: [d for d in found if not d[3]] for axis, found in digits.items()}
    near = [d for d in layout if d[3]]
    one = tuple(far["mats"] + far["tp"] + near)
    two = tuple(far["mats"][:1] + far["tp"] + far["mats"][1:] + near)
    return layout, [one, two] if one != two else [one]


def per_device(scale, digits, grad, momentum):
    new_momentum = momentum_beta * momentum + grad.astype(jnp.float32)
    iterate = (grad.astype(jnp.float32) + momentum_beta * new_momentum).astype(jnp.bfloat16)
    layout, orders = orders_of(digits)
    lines = {axis: tuple(sorted(found, key=lambda d: d[3])) for axis, found in digits.items()}
    size = momentum.shape[0] * lax.axis_size("tp")
    mine = iterate.shape[0]
    block = math.gcd(mine, 256)
    window = window_of(size // block) * block
    smem = pl.BlockSpec(memory_space=pltpu.SMEM)
    whole = pl.BlockSpec(memory_space=pltpu.VMEM)
    params = pltpu.CompilerParams(vmem_limit_bytes=grant)
    tp = lax.axis_index("tp")
    fused = reduced_gram(iterate, digits, block, window, 1)
    if fused is not None:
        columns, share = fused
    else:
        columns = gather(iterate, "tp", tuple(digits["tp"]), [lines["tp"]], 6, 1, "gather_x")
        part = pl.pallas_call(
            functools.partial(gram_kernel, block),
            out_shape=jax.ShapeDtypeStruct((mine, window), jnp.bfloat16),
            in_specs=[smem, whole],
            out_specs=whole,
            compiler_params=params,
            name="gram",
        )(tp.reshape(1), columns)
        share = lax.psum_scatter(part, "mats", scatter_dimension=0, tiled=True)
    if fused is not None:
        update = finished(share, columns, digits, block, scale, 2)
        if update is not None:
            return (update, new_momentum)
    compact = gather(share, ("tp", "mats"), layout, orders, 2, 2, "gather_gram")
    count = share.shape[0]
    place = tp * lax.axis_size("mats") + lax.axis_index("mats")
    thin = pltpu.VMEM((count, size), jnp.bfloat16)
    rows, kappa = pl.pallas_call(
        functools.partial(poly_kernel, block, scale),
        out_shape=(
            jax.ShapeDtypeStruct((count, size), jnp.bfloat16),
            jax.ShapeDtypeStruct((1, 128), jnp.float32),
        ),
        in_specs=[smem, whole],
        out_specs=(whole, whole),
        scratch_shapes=[pltpu.VMEM((size, size), jnp.bfloat16)] + [thin] * 5,
        compiler_params=params,
        cost_estimate=pl.CostEstimate(
            flops=22 * count * size * size, bytes_accessed=size * window * 2, transcendentals=0
        ),
        name="poly",
    )(place.reshape(1), compact)
    matrix = gather(rows, "mats", tuple(digits["mats"]), [lines["mats"]], 3, 3, "gather_rows")
    product = jnp.dot(matrix, columns, preferred_element_type=jnp.float32)
    update = (product + kappa[0, 0] * iterate.astype(jnp.float32)).astype(jnp.bfloat16)
    return (update, new_momentum)


def solution(mesh):
    digits = digits_of(mesh)

    def step(grad, momentum):
        scale = shape_gain * math.sqrt(max(grad.shape))
        return jax.shard_map(
            functools.partial(per_device, scale, digits),
            mesh=mesh,
            in_specs=(P("tp", "mats"), P("tp", "mats")),
            out_specs=(P("tp", "mats"), P("tp", "mats")),
            check_vma=False,
        )(grad, momentum)

    return step
```

```python
import functools
import math

import jax
import jax.numpy as jnp
from jax import lax
from jax.experimental import pallas as pl
from jax.experimental.pallas import tpu as pltpu
from jax.sharding import PartitionSpec as P

momentum_beta = 0.95
first_coef = 3.4445
second_coef = -4.775
third_coef = 2.0315
shape_gain = 0.2
epsilon = 1e-06
grant = 62 * 1024 * 1024


def digits_of(mesh):
    table = {}
    shape = mesh.devices.shape
    for number, axis in enumerate(mesh.axis_names):
        extent = shape[number]
        line = [mesh.devices[tuple(i if k == number else 0 for k in range(len(shape)))] for i in range(extent)]
        found = []
        if all(hasattr(device, "coords") for device in line):
            places = [(*device.coords, device.core_on_chip) for device in line]
            for place, column in enumerate(zip(*places)):
                kinds = len(set(column))
                if kinds > 1:
                    stride = next(i for i in range(extent) if column[i] != column[0])
                    if all((i // stride) % kinds == column[i] - column[0] for i in range(extent)):
                        found.append((axis, stride, kinds, place == 3))
        if math.prod(kinds for _, _, kinds, _ in found) != extent:
            found = [(axis, 1, extent, False)]
        table[axis] = sorted(found, key=lambda digit: -digit[1])
    return table


def place(digit):
    axis, stride, extent, _ = digit
    return lax.rem(lax.div(lax.axis_index(axis), stride), extent)


def moves(digit):
    here, extent = place(digit), digit[2]
    if extent == 2:
        return [(1 - 2 * here, None)]
    return [(1, here + 1 < extent), (-1, here >= 1)]


def when(condition, body):
    if condition is None:
        body()
    else:
        pl.when(condition)(body)


def both(*conditions):
    found = [c for c in conditions if c is not None]
    return functools.reduce(lambda a, b: a & b, found) if found else None


def peer(digit, offset):
    axis, stride, _, _ = digit
    return {axis: lax.axis_index(axis) + offset * stride}


def barrier_all(digits):
    semaphore = pltpu.get_barrier_semaphore()
    for digit in digits:
        for offset, has in moves(digit):
            when(has, functools.partial(
                pl.semaphore_signal, semaphore, inc=1, device_id=peer(digit, offset),
                device_id_type=pl.DeviceIdType.MESH))
    count = 0
    for digit in digits:
        for _, has in moves(digit):
            count = count + (1 if has is None else has.astype(jnp.int32))
    pl.semaphore_wait(semaphore, count)


def around(digit, step):
    here = place(digit)
    there = lax.rem(here + step, digit[2])
    return there, there - here


def barrier_lines(digits):
    semaphore = pltpu.get_barrier_semaphore()
    count = 0
    for digit in digits:
        for step in range(1, digit[2]):
            _, offset = around(digit, step)
            pl.semaphore_signal(
                semaphore, inc=1, device_id=peer(digit, offset),
                device_id_type=pl.DeviceIdType.MESH,
            )
            count += 1
    pl.semaphore_wait(semaphore, count)


def relatives(digit):
    here, extent = place(digit), digit[2]
    if extent == 2:
        return [(1, 0, 1 - here, None)]
    found = []
    for hop in range(1, extent):
        found.append((hop, 1, here - hop, here >= hop))
        found.append((hop, -1, here + hop, here + hop < extent))
    return found


class Gather:
    def __init__(self, layout, pieces, buffer, source, send_sem, recv_sem):
        self.layout, self.pieces, self.buffer, self.source = layout, pieces, buffer, source
        self.send_sem, self.recv_sem = send_sem, recv_sem
        self.sent = {}

    @staticmethod
    def semaphores(layout, pieces):
        dims = tuple(d[2] for d in layout)
        return [
            pltpu.SemaphoreType.DMA((len(pieces), 2 * len(layout)) + dims),
            pltpu.SemaphoreType.DMA((len(pieces),) + dims),
        ]

    def copy(self, piece, block, digit, offset, way, own):
        order, row, count = self.pieces[piece]
        index = tuple(block[d] for d in self.layout)
        rows = (pl.ds(row, count), slice(None))
        at = self.buffer.at[index + rows]
        lane = 2 * self.layout.index(digit) + way
        return pltpu.make_async_remote_copy(
            src_ref=self.source.at[rows] if own else at,
            dst_ref=at,
            send_sem=self.send_sem.at[(piece, lane) + index],
            recv_sem=self.recv_sem.at[(piece,) + index],
            device_id=peer(digit, offset),
            device_id_type=pl.DeviceIdType.MESH,
        )

    def send(self, piece, block, exists, digit, directions, tag, own=False):
        for way, (offset, has) in enumerate(moves(digit)):
            if directions is not None and way not in directions:
                continue
            copy = self.copy(piece, block, digit, offset, way, own)
            condition = both(exists, has)
            when(condition, copy.start)
            self.sent[(piece, tag, digit, way)] = (block, exists, own)

    def events(self, piece):
        order = self.pieces[piece][0]
        here = {d: place(d) for d in order}
        found = []

        def begin(after):
            for digit in order:
                self.send(piece, here, None, digit, None, (), own=True)

        found.append((0, begin, ()))

        def arrivals(stage, block, exists, tag, depth):
            digit = order[stage]
            for hop, travel, q, there in relatives(digit):
                source = {**block, digit: q}
                condition = both(exists, there)
                label = tag + ((digit, hop, travel),)

                def arrive(after, source=source, condition=condition, travel=travel, label=label):
                    offset, _ = moves(digit)[0]
                    when(condition, self.copy(piece, source, digit, offset, 0, False).wait_recv)
                    if digit[2] > 2:
                        self.send(piece, source, condition, digit, (0 if travel > 0 else 1,), label)
                    for later in order[stage + 1 :]:
                        self.send(piece, source, condition, later, None, label)
                    if after is not None:
                        after(piece, source, condition, label)

                found.append((depth + hop, arrive, label))

        def expand(stage, earlier, block, exists, tag, depth):
            if earlier == stage:
                arrivals(stage, block, exists, tag, depth)
                return
            digit = order[earlier]
            expand(stage, earlier + 1, {**block, digit: here[digit]}, exists, tag, depth)
            for hop, travel, q, there in relatives(digit):
                expand(
                    stage, earlier + 1, {**block, digit: q}, both(exists, there),
                    tag + ((digit, hop, travel),), depth + hop,
                )

        for stage in range(len(order)):
            expand(stage, 0, dict(here), None, (), 0)
        return found

    def queue(self):
        entries = []
        for piece in range(len(self.pieces)):
            for depth, action, tag in self.events(piece):
                entries.append((depth, piece, len(entries), action, tag))
        entries.sort(key=lambda entry: entry[:3])
        return [(piece, action, tag) for _, piece, _, action, tag in entries]

    def run(self, after=None):
        for _, action, _ in self.queue():
            action(after)

    def drain(self):
        for (piece, _, digit, way), (block, exists, own) in self.sent.items():
            offset, has = moves(digit)[way]
            copy = self.copy(piece, block, digit, offset, way, own)
            when(both(exists, has), copy.wait_send)


def gather_kernel(layout, pieces, x_ref, out_ref, send_sem, recv_sem, local_sem):
    barrier_all(layout)
    gather = Gather(layout, pieces, out_ref, x_ref, send_sem, recv_sem)
    gather.run()
    local = pltpu.make_async_copy(x_ref, out_ref.at[tuple(place(d) for d in layout)], local_sem)
    local.start()
    local.wait()
    gather.drain()


def pieces_of(rows, orders, chunks):
    units = max(1, rows // 16)
    chunks = min(chunks, units)
    cuts = [units * i // chunks * 16 for i in range(chunks)] + [rows]
    return [(orders[i % len(orders)], cuts[i], cuts[i + 1] - cuts[i]) for i in range(chunks)]


def events_of(order):
    total, held = 0, 1
    for digit in order:
        around = 1 if digit[2] == 2 else 2 * (digit[2] - 1)
        total += held * around
        held *= 1 + around
    return total


def gather(x, axes, layout, orders, chunks, ident, name):
    rows, columns = x.shape
    if rows % 16 or len(orders) * events_of(orders[0]) > 256:
        return lax.all_gather(x, axes, axis=0, tiled=True)
    pieces = pieces_of(rows, orders, chunks)
    dims = tuple(d[2] for d in layout)
    out = pl.pallas_call(
        functools.partial(gather_kernel, layout, pieces),
        out_shape=jax.ShapeDtypeStruct(dims + (rows, columns), x.dtype),
        in_specs=[pl.BlockSpec(memory_space=pltpu.VMEM)],
        out_specs=pl.BlockSpec(memory_space=pl.ANY),
        scratch_shapes=Gather.semaphores(layout, pieces) + [pltpu.SemaphoreType.DMA],
        compiler_params=pltpu.CompilerParams(collective_id=ident, has_side_effects=True),
        name=name,
    )(x)
    return out.reshape(math.prod(dims) * rows, columns)


def nt_dot(left, right):
    return lax.dot_general(
        left, right, (((1,), (1,)), ((), ())), preferred_element_type=jnp.float32
    )


def window_of(blocks):
    return blocks // 2 + 1


def gram_kernel(block, where_ref, x_ref, part_ref):
    blocks = x_ref.shape[0] // block
    mine = part_ref.shape[0] // block
    window = part_ref.shape[1] // block
    first = where_ref[0] * mine
    left_at = pl.ds(pl.multiple_of(first * block, block), mine * block)
    for j in range(mine + window - 1):
        low, high = max(0, j - window + 1), min(mine - 1, j)
        other = lax.rem(first + j, blocks)
        right = x_ref[pl.ds(pl.multiple_of(other * block, block), block), :]
        rows = pl.ds(
            pl.multiple_of((first + low) * block, block), (high - low + 1) * block
        )
        product = nt_dot(x_ref[rows, :], right).astype(jnp.bfloat16)
        for i in range(low, high + 1):
            at = (i - low) * block
            part_ref[i * block : (i + 1) * block, (j - i) * block : (j - i + 1) * block] = (
                product[at : at + block, :]
            )


def reduce_kernel(
    block, rows, pieces, far, near, x_ref, columns_ref, share_ref, held, part, got_near, half, got_far,
    send_sem, recv_sem, near_send, near_recv, far_send, far_recv, out_sem,
):
    order = pieces[0][0]
    layout = tuple(sorted(order, key=lambda d: -d[1]))
    shards = math.prod(d[2] for d in layout)
    mine = x_ref.shape[0] // block
    total = part.shape[0]
    window = total - mine + 1
    lines = far[2]
    axis = layout[0][0]
    shard = lax.axis_index(axis)
    barrier_lines(layout + (far, near))
    gather = Gather(layout, pieces, held, x_ref, send_sem, recv_sem)
    queue = gather.queue()
    starts = [entry for entry in queue if not entry[2]]
    events = [entry for entry in queue if entry[2]]

    def home(t, tag):
        for digit, _, _ in tag:
            _, stride, _, _ = digit
            t = t - stride if (t // stride) % 2 else t + stride
        return t

    arrival = sorted(range(total), key=lambda j: (j // mine > 0, j % mine if j // mine else j, j // mine))

    def needed(t, j):
        s, piece = j // mine % shards, j % mine
        return {((t + s) % shards, piece)} if s else set()

    slots = [[] for _ in range(total + 1)]
    done = [0] * shards
    early = []
    for k in range(total + 1):
        begun = {}
        for t in range(shards):
            last = len(events)
            if k < total:
                wanted = needed(t, arrival[k])
                last = max(
                    [done[t]]
                    + [e + 1 for e, (piece, _, tag) in enumerate(events) if (home(t, tag), piece) in wanted]
                )
            if k == total - 1 and last == done[t]:
                early.append(t)
            for e in range(done[t], last):
                begun.setdefault(e, []).append(t)
            done[t] = last
        slots[k] = sorted(begun.items())
    copies = {}

    def keep(piece, source, condition, tag):
        _, row, count = pieces[piece]
        at = tuple(source[d] for d in layout) + (pl.ds(row, count), slice(None))
        number = next(e for e, entry in enumerate(events) if entry[0] == piece and entry[2] == tag)
        copies[number] = at
        pltpu.make_async_copy(held.at[at], columns_ref.at[at], out_sem.at[number]).start()

    for _, action, _ in starts:
        action(None)
    own = pltpu.make_async_copy(
        x_ref, columns_ref.at[tuple(place(d) for d in layout)], out_sem.at[len(events)]
    )
    own.start()

    def advance(d):
        for e, who in slots[d]:
            _, action, _ = events[e]
            if len(who) == shards:
                action(keep)
            else:
                condition = functools.reduce(lambda a, b: a | b, [shard == t for t in who])
                pl.when(condition)(functools.partial(action, keep))

    def span(j):
        low, high = max(0, j - window + 1), min(mine - 1, j)
        return low, high - low + 1

    def near_copy(j):
        blocks = pl.ds(*span(j))
        return pltpu.make_async_remote_copy(
            src_ref=part.at[j, blocks, :, 1 - place(near)],
            dst_ref=got_near.at[j, blocks],
            send_sem=near_send.at[j],
            recv_sem=near_recv.at[j],
            device_id=peer(near, 1 - 2 * place(near)),
            device_id_type=pl.DeviceIdType.MESH,
        )

    def far_copy(j, step, arriving):
        there, offset = around(far, step)
        slot = there if arriving else place(far)
        blocks = pl.ds(*span(j))
        return pltpu.make_async_remote_copy(
            src_ref=half.at[j, there, blocks],
            dst_ref=got_far.at[j, slot, blocks],
            send_sem=far_send.at[j, there],
            recv_sem=far_recv.at[j, slot],
            device_id=peer(far, offset),
            device_id_type=pl.DeviceIdType.MESH,
        )

    def form(k):
        j = arrival[k]
        s, piece = j // mine % shards, j % mine
        at = (pl.ds(piece * block, block), slice(None))
        if s:
            other = lax.rem(shard + s, shards)
            at = tuple(lax.rem(lax.div(other, g[1]), g[2]) for g in layout) + at
            right = held[at]
        else:
            right = x_ref[at]
        low, size = span(j)
        product = nt_dot(x_ref[low * block : (low + size) * block, :], right).astype(jnp.bfloat16)
        for i in range(low, low + size):
            row = (i - low) * block
            part[j, i] = product[row : row + block, :].reshape(lines, near[2], rows, block)
        near_copy(j).start()

    def halve(j):
        low, size = span(j)
        near_copy(j).wait_recv()
        for i in range(low, low + size):
            for line in range(lines):
                half[j, line, i] = (
                    part[j, i, line, place(near)].astype(jnp.float32)
                    + got_near[j, i, line].astype(jnp.float32)
                ).astype(jnp.bfloat16)
        for step in range(1, lines):
            far_copy(j, step, False).start()

    def finish(j):
        low, size = span(j)
        for step in range(1, lines):
            far_copy(j, step, True).wait_recv()
        for i in range(low, low + size):
            value = half[j, place(far), i].astype(jnp.float32)
            for step in range(1, lines):
                there, _ = around(far, step)
                value = value + got_far[j, there, i].astype(jnp.float32)
            d = j - i
            share_ref[i * rows : (i + 1) * rows, d * block : (d + 1) * block] = value.astype(jnp.bfloat16)

    def among(who):
        return functools.reduce(lambda a, b: a | b, [shard == t for t in who])

    split = bool(early) and len(early) < shards
    for k in range(total):
        if k > 0:
            halve(arrival[k - 1])
        if k > 1:
            finish(arrival[k - 2])
        advance(k)
        if k == total - 1 and split:
            pl.when(jnp.logical_not(among(early)))(functools.partial(form, k))
        else:
            form(k)
        if k == total - 2 and split:
            pl.when(among(early))(functools.partial(form, total - 1))
    halve(arrival[total - 1])
    for j in arrival[-2:]:
        finish(j)
    advance(total)

    for j in range(total):
        near_copy(j).wait_send()
        for step in range(1, lines):
            far_copy(j, step, False).wait_send()
    for number, at in copies.items():
        pltpu.make_async_copy(held.at[at], columns_ref.at[at], out_sem.at[number]).wait()
    own.wait()
    gather.drain()


def reduced_gram(iterate, digits, block, window, ident):
    layout = tuple(digits["tp"])
    far, near = digits["mats"]
    mine, width = iterate.shape
    rows = block // (far[2] * near[2])
    order = tuple(sorted(layout, key=lambda d: d[3]))
    pieces = [(order, row, block) for row in range(0, mine, block)]
    dims = tuple(d[2] for d in layout)
    own = mine // block
    total, lines = window // block + own - 1, far[2]
    near_tile = pltpu.VMEM((total, own, lines, rows, block), jnp.bfloat16)
    far_tile = pltpu.VMEM((total, lines, own, rows, block), jnp.bfloat16)
    dma = pltpu.SemaphoreType.DMA
    blocks = math.prod(dims) - 1
    columns, share = pl.pallas_call(
        functools.partial(reduce_kernel, block, rows, pieces, far, near),
        out_shape=(
            jax.ShapeDtypeStruct(dims + iterate.shape, jnp.bfloat16),
            jax.ShapeDtypeStruct((own * rows, window), jnp.bfloat16),
        ),
        in_specs=[pl.BlockSpec(memory_space=pltpu.VMEM)],
        out_specs=(pl.BlockSpec(memory_space=pl.ANY), pl.BlockSpec(memory_space=pltpu.VMEM)),
        scratch_shapes=[
            pltpu.VMEM(dims + iterate.shape, jnp.bfloat16),
            pltpu.VMEM((total, own, lines, near[2], rows, block), jnp.bfloat16),
            near_tile, far_tile, far_tile,
        ]
        + Gather.semaphores(layout, pieces)
        + [dma((total,))] * 2
        + [dma((total, lines))] * 2
        + [dma((blocks * len(pieces) + 1,))],
        compiler_params=pltpu.CompilerParams(
            collective_id=ident, has_side_effects=True, vmem_limit_bytes=grant
        ),
        name="reduced_gram",
    )(iterate)
    return columns.reshape(dims[0] * math.prod(dims[1:]) * mine, width), share


def polynomial_rows(gram, own, one, two, left, right, raw, sums, scale, where_ref):
    size = gram.shape[0]
    count = own.shape[0]
    width = math.gcd(size, 1024)
    def columns(body):
        @pl.loop(0, size // width)
        def _(step):
            body(pl.ds(pl.multiple_of(step * width, width), width))

    if where_ref is None:
        pass
    elif count % 16 == 0:
        own[...] = gram[pl.ds(pl.multiple_of(where_ref[0] * count, 16), count), :]
    else:
        row = lax.broadcasted_iota(jnp.int32, (count, size), 0) + where_ref[0] * count
        column = lax.broadcasted_iota(jnp.int32, (count, size), 1)
        two[...] = (row == column).astype(jnp.float32).astype(jnp.bfloat16)

        def select(at):
            own[:, at] = jnp.dot(
                two[...], gram[:, at], preferred_element_type=jnp.float32
            ).astype(jnp.bfloat16)

        columns(select)

    tile = math.gcd(size, 512)

    @pl.loop(0, size // tile)
    def _(step):
        at = pl.ds(pl.multiple_of(step * tile, tile), tile)
        raw[:, at] = jnp.dot(own[...], gram[:, at], preferred_element_type=jnp.float32)
        sums[:, at] = jnp.sum(jnp.abs(gram[:, at].astype(jnp.float32)), axis=0, keepdims=True)

    bound = jnp.max(sums[...], axis=1, keepdims=True) + epsilon
    root = lax.rsqrt(jnp.broadcast_to(bound, (1, 128)))
    inverse = (root * root)[:, :1]

    def times_gram(source, at):
        return inverse * jnp.dot(source[...], gram[:, at], preferred_element_type=jnp.float32)

    def wide(ref, at):
        return ref[:, at].astype(jnp.float32)

    def apply(source, target, constant=None):
        def body(at):
            value = times_gram(source, at)
            if constant is not None:
                value = value + (constant * inverse) * wide(own, at)
            target[:, at] = value.astype(jnp.bfloat16)

        columns(body)

    def polynomial(source, middle, target):
        apply(source, middle)

        def body(at):
            target[:, at] = (
                first_coef * wide(source, at)
                + second_coef * wide(middle, at)
                + third_coef * times_gram(middle, at)
            ).astype(jnp.bfloat16)

        columns(body)

    def first(at):
        one[:, at] = (
            second_coef * (inverse * wide(own, at)) + third_coef * (inverse * (inverse * raw[:, at]))
        ).astype(jnp.bfloat16)

    columns(first)
    apply(one, left, first_coef)
    polynomial(left, right, two)
    polynomial(two, right, left)

    def keep(at):
        two[:, at] = left[:, at]

    columns(keep)
    apply(two, right)
    polynomial(right, left, own)
    polynomial(own, left, right)

    def finish(at):
        mixed = (
            first_coef * wide(one, at) + second_coef * wide(two, at) + third_coef * wide(right, at)
        )
        left[:, at] = ((scale * root[:, :1]) * mixed).astype(jnp.bfloat16)

    columns(finish)
    return root


def poly_kernel(block, scale, where_ref, compact_ref, out_ref, kappa_ref, gram, own, one, two, left, right, raw, sums):
    size = gram.shape[0]
    blocks = size // block
    window = compact_ref.shape[1] // block
    for i in range(blocks):
        for d in range(window):
            j = (i + d) % blocks
            tile = compact_ref[i * block : (i + 1) * block, d * block : (d + 1) * block]
            gram[i * block : (i + 1) * block, j * block : (j + 1) * block] = tile
            if d > 0 and 2 * d != blocks:
                gram[j * block : (j + 1) * block, i * block : (i + 1) * block] = tile.T

    root = polynomial_rows(gram, own, one, two, left, right, raw, sums, scale, where_ref)
    kappa_ref[...] = (scale * first_coef * first_coef) * root
    out_ref[...] = left[...]


def finish_kernel(
    block, scale, layout, pieces, near_pieces, share_ref, columns_ref, out_ref, held, gram, own, one, two, left,
    right, raw, sums, rows, columns, result, send_sem, recv_sem, rows_send, rows_recv, in_sem, out_sem,
):
    barrier_all(layout)
    tp = tuple(d for d in layout if d[0] == "tp")
    far, near = (d for d in layout if d[0] == "mats")
    load = pltpu.make_async_copy(columns_ref, columns, in_sem)
    gather = Gather(layout, pieces, held, share_ref, send_sem, recv_sem)
    queue = gather.queue()
    for _, action, tag in queue:
        if not tag:
            action(None)
    load.start()
    held[tuple(place(d) for d in layout)] = share_ref[...]
    for _, action, tag in queue:
        if tag:
            action(None)

    size = gram.shape[0]
    count, window = share_ref.shape
    blocks = size // block
    shards = math.prod(d[2] for d in tp)
    mine = size // shards
    own_blocks = mine // block
    seg = count // own_blocks
    for t in range(shards):
        at = tuple((t // d[1]) % d[2] for d in tp)
        for d in range(window // block):
            for k in range(own_blocks):
                i = t * own_blocks + k
                j = (i + d) % blocks
                tile = held[at + (slice(None), slice(None), pl.ds(k * seg, seg), pl.ds(d * block, block))]
                tile = tile.reshape(block, block)
                gram[i * block : (i + 1) * block, j * block : (j + 1) * block] = tile
                if d > 0 and 2 * d != blocks:
                    gram[j * block : (j + 1) * block, i * block : (i + 1) * block] = tile.T

    first = lax.axis_index("tp") * mine + lax.axis_index("mats") * seg
    for k in range(own_blocks):
        at = pl.ds(pl.multiple_of(first + k * block, 16), seg)
        own[k * seg : (k + 1) * seg, :] = gram[at, :]
    root = polynomial_rows(gram, own, one, two, left, right, raw, sums, scale, None)
    kappa = ((scale * first_coef * first_coef) * root)[:, :1]

    spread = Gather((far, near), near_pieces, rows, left, rows_send, rows_recv)
    queue = spread.queue()
    for _, action, tag in queue:
        if not tag:
            action(None)
    rows[place(far), place(near)] = left[...]
    load.wait()
    pair = near[2] * count
    width = math.gcd(columns.shape[1], 512)
    shard_row = lax.axis_index("tp") * mine

    def multiply(line):
        matrix = rows[line].reshape(pair, size)

        @pl.loop(0, columns.shape[1] // width)
        def _(step):
            across = pl.ds(pl.multiple_of(step * width, width), width)
            product = jnp.dot(matrix, columns[:, across], preferred_element_type=jnp.float32)
            for n in range(near[2]):
                for k in range(own_blocks):
                    start = shard_row + k * block + (line * near[2] + n) * seg
                    mirror = columns[pl.ds(pl.multiple_of(start, 16), seg), across]
                    row = n * count + k * seg
                    result[k, line, n * seg : (n + 1) * seg, across] = (
                        product[row : row + seg, :] + kappa * mirror.astype(jnp.float32)
                    ).astype(jnp.bfloat16)

        pltpu.make_async_copy(result.at[:, line], out_ref.at[:, line], out_sem.at[line]).start()

    groups = [(None, place(far), None)]
    groups += [((far, hop, travel), q, there) for hop, travel, q, there in relatives(far)]
    missing = []
    for label, q, there in groups:
        wanted = set()
        for piece, _, tag in queue:
            if tag and [part for part in tag if part[0] == far] == ([label] if label else []):
                wanted.add((piece, tag))
        missing.append((wanted, q, there))
    for piece, action, tag in queue:
        if not tag:
            continue
        action(None)
        for wanted, q, there in missing:
            if (piece, tag) in wanted:
                wanted.remove((piece, tag))
                if not wanted:
                    when(there, functools.partial(multiply, q))
    for line in range(far[2]):
        pltpu.make_async_copy(result.at[:, line], out_ref.at[:, line], out_sem.at[line]).wait()
    gather.drain()
    spread.drain()


def finished(share, columns, digits, block, scale, ident):
    layout, _ = orders_of(digits)
    count, window = share.shape
    far, near = digits["mats"]
    side = [d for d in digits["tp"] if not d[3]]
    close = tuple(d for d in digits["tp"] if d[3])
    orders = [(far, near, side[0]) + close, (far, side[0], near) + close]
    pieces = pieces_of(count, orders, 2)
    most = (count * 5 // 6 + 15) // 16 * 16
    near_pieces = [((far, near), 0, most)]
    if most < count:
        near_pieces.append(((near, far), most, count - most))
    size, width = columns.shape
    dims = tuple(d[2] for d in layout)
    mine = count * far[2] * near[2]
    thin = pltpu.VMEM((count, size), jnp.bfloat16)
    shape = (mine // block, far[2], block // far[2], width)
    return pl.pallas_call(
        functools.partial(finish_kernel, block, scale, layout, pieces, near_pieces),
        out_shape=jax.ShapeDtypeStruct(shape, jnp.bfloat16),
        in_specs=[pl.BlockSpec(memory_space=pltpu.VMEM), pl.BlockSpec(memory_space=pl.ANY)],
        out_specs=pl.BlockSpec(memory_space=pl.ANY),
        scratch_shapes=[
            pltpu.VMEM(dims + share.shape, jnp.bfloat16),
            pltpu.VMEM((size, size), jnp.bfloat16),
        ]
        + [thin] * 5
        + [
            pltpu.VMEM((count, size), jnp.float32),
            pltpu.VMEM((1, size), jnp.float32),
            pltpu.VMEM((far[2], near[2], count, size), jnp.bfloat16),
            pltpu.VMEM((size, width), jnp.bfloat16),
            pltpu.VMEM(shape, jnp.bfloat16),
        ]
        + Gather.semaphores(layout, pieces)
        + Gather.semaphores((far, near), near_pieces)
        + [pltpu.SemaphoreType.DMA, pltpu.SemaphoreType.DMA((far[2],))],
        compiler_params=pltpu.CompilerParams(
            collective_id=ident, has_side_effects=True, vmem_limit_bytes=63 * 1024 * 1024
        ),
        name="finished",
    )(share, columns).reshape(mine, width)


def paired(digits, block):
    tp, mats = digits["tp"], digits["mats"]
    if len(tp) != 2 or len(mats) != 2 or mats[1][2] != 2 or any(d[2] != 2 for d in tp):
        return False
    if sum(not d[3] for d in tp) != 1:
        return False
    return block % (16 * mats[0][2] * mats[1][2]) == 0


def orders_of(digits):
    layout = tuple(digits["tp"]) + tuple(digits["mats"])
    far = {axis: [d for d in found if not d[3]] for axis, found in digits.items()}
    near = [d for d in layout if d[3]]
    one = tuple(far["mats"] + far["tp"] + near)
    two = tuple(far["mats"][:1] + far["tp"] + far["mats"][1:] + near)
    return layout, [one, two] if one != two else [one]


def per_device(scale, digits, grad, momentum):
    new_momentum = momentum_beta * momentum + grad.astype(jnp.float32)
    iterate = (grad.astype(jnp.float32) + momentum_beta * new_momentum).astype(jnp.bfloat16)
    layout, orders = orders_of(digits)
    lines = {axis: tuple(sorted(found, key=lambda d: d[3])) for axis, found in digits.items()}
    size = momentum.shape[0] * lax.axis_size("tp")
    mine = iterate.shape[0]
    block = math.gcd(mine, 256)
    window = window_of(size // block) * block
    smem = pl.BlockSpec(memory_space=pltpu.SMEM)
    whole = pl.BlockSpec(memory_space=pltpu.VMEM)
    params = pltpu.CompilerParams(vmem_limit_bytes=grant)
    tp = lax.axis_index("tp")
    if paired(digits, block):
        columns, share = reduced_gram(iterate, digits, block, window, 1)
        return (finished(share, columns, digits, block, scale, 2), new_momentum)
    columns = gather(iterate, "tp", tuple(digits["tp"]), [lines["tp"]], 6, 1, "gather_x")
    part = pl.pallas_call(
        functools.partial(gram_kernel, block),
        out_shape=jax.ShapeDtypeStruct((mine, window), jnp.bfloat16),
        in_specs=[smem, whole],
        out_specs=whole,
        compiler_params=params,
        name="gram",
    )(tp.reshape(1), columns)
    share = lax.psum_scatter(part, "mats", scatter_dimension=0, tiled=True)
    compact = gather(share, ("tp", "mats"), layout, orders, 2, 2, "gather_gram")
    count = share.shape[0]
    place = tp * lax.axis_size("mats") + lax.axis_index("mats")
    thin = pltpu.VMEM((count, size), jnp.bfloat16)
    rows, kappa = pl.pallas_call(
        functools.partial(poly_kernel, block, scale),
        out_shape=(
            jax.ShapeDtypeStruct((count, size), jnp.bfloat16),
            jax.ShapeDtypeStruct((1, 128), jnp.float32),
        ),
        in_specs=[smem, whole],
        out_specs=(whole, whole),
        scratch_shapes=[pltpu.VMEM((size, size), jnp.bfloat16)]
        + [thin] * 5
        + [pltpu.VMEM((count, size), jnp.float32), pltpu.VMEM((1, size), jnp.float32)],
        compiler_params=params,
        cost_estimate=pl.CostEstimate(
            flops=22 * count * size * size, bytes_accessed=size * window * 2, transcendentals=0
        ),
        name="poly",
    )(place.reshape(1), compact)
    matrix = gather(rows, "mats", tuple(digits["mats"]), [lines["mats"]], 3, 3, "gather_rows")
    product = jnp.dot(matrix, columns, preferred_element_type=jnp.float32)
    update = (product + kappa[0, 0] * iterate.astype(jnp.float32)).astype(jnp.bfloat16)
    return (update, new_momentum)


def solution(mesh):
    digits = digits_of(mesh)

    def step(grad, momentum):
        scale = shape_gain * math.sqrt(max(grad.shape))
        return jax.shard_map(
            functools.partial(per_device, scale, digits),
            mesh=mesh,
            in_specs=(P("tp", "mats"), P("tp", "mats")),
            out_specs=(P("tp", "mats"), P("tp", "mats")),
            check_vma=False,
        )(grad, momentum)

    return step
```

```python
import functools
import math

import jax
import jax.numpy as jnp
from jax import lax
from jax.experimental import pallas as pl
from jax.experimental.pallas import tpu as pltpu
from jax.sharding import PartitionSpec as P

momentum_beta = 0.95
first_coef = 3.4445
second_coef = -4.775
third_coef = 2.0315
shape_gain = 0.2
epsilon = 1e-06
grant = 62 * 1024 * 1024


def digits_of(mesh):
    table = {}
    shape = mesh.devices.shape
    for number, axis in enumerate(mesh.axis_names):
        extent = shape[number]
        line = [mesh.devices[tuple(i if k == number else 0 for k in range(len(shape)))] for i in range(extent)]
        found = []
        if all(hasattr(device, "coords") for device in line):
            places = [(*device.coords, device.core_on_chip) for device in line]
            for place, column in enumerate(zip(*places)):
                kinds = len(set(column))
                if kinds > 1:
                    stride = next(i for i in range(extent) if column[i] != column[0])
                    if all((i // stride) % kinds == column[i] - column[0] for i in range(extent)):
                        found.append((axis, stride, kinds, place == 3))
        if math.prod(kinds for _, _, kinds, _ in found) != extent:
            found = [(axis, 1, extent, False)]
        table[axis] = sorted(found, key=lambda digit: -digit[1])
    return table


def place(digit):
    axis, stride, extent, _ = digit
    return lax.rem(lax.div(lax.axis_index(axis), stride), extent)


def moves(digit):
    here, extent = place(digit), digit[2]
    if extent == 2:
        return [(1 - 2 * here, None)]
    return [(1, here + 1 < extent), (-1, here >= 1)]


def when(condition, body):
    if condition is None:
        body()
    else:
        pl.when(condition)(body)


def both(*conditions):
    found = [c for c in conditions if c is not None]
    return functools.reduce(lambda a, b: a & b, found) if found else None


def peer(digit, offset):
    axis, stride, _, _ = digit
    return {axis: lax.axis_index(axis) + offset * stride}


def barrier_all(digits):
    semaphore = pltpu.get_barrier_semaphore()
    for digit in digits:
        for offset, has in moves(digit):
            when(has, functools.partial(
                pl.semaphore_signal, semaphore, inc=1, device_id=peer(digit, offset),
                device_id_type=pl.DeviceIdType.MESH))
    count = 0
    for digit in digits:
        for _, has in moves(digit):
            count = count + (1 if has is None else has.astype(jnp.int32))
    pl.semaphore_wait(semaphore, count)


def around(digit, step):
    here = place(digit)
    there = lax.rem(here + step, digit[2])
    return there, there - here


def barrier_lines(digits):
    semaphore = pltpu.get_barrier_semaphore()
    count = 0
    for digit in digits:
        for step in range(1, digit[2]):
            _, offset = around(digit, step)
            pl.semaphore_signal(
                semaphore, inc=1, device_id=peer(digit, offset),
                device_id_type=pl.DeviceIdType.MESH,
            )
            count += 1
    pl.semaphore_wait(semaphore, count)


def relatives(digit):
    here, extent = place(digit), digit[2]
    if extent == 2:
        return [(1, 0, 1 - here, None)]
    found = []
    for hop in range(1, extent):
        found.append((hop, 1, here - hop, here >= hop))
        found.append((hop, -1, here + hop, here + hop < extent))
    return found


class Gather:
    def __init__(self, layout, pieces, buffer, source, send_sem, recv_sem):
        self.layout, self.pieces, self.buffer, self.source = layout, pieces, buffer, source
        self.send_sem, self.recv_sem = send_sem, recv_sem
        self.sent = {}

    @staticmethod
    def semaphores(layout, pieces):
        dims = tuple(d[2] for d in layout)
        return [
            pltpu.SemaphoreType.DMA((len(pieces), 2 * len(layout)) + dims),
            pltpu.SemaphoreType.DMA((len(pieces),) + dims),
        ]

    def copy(self, piece, block, digit, offset, way, own):
        order, row, count = self.pieces[piece]
        index = tuple(block[d] for d in self.layout)
        rows = (pl.ds(row, count), slice(None))
        at = self.buffer.at[index + rows]
        lane = 2 * self.layout.index(digit) + way
        return pltpu.make_async_remote_copy(
            src_ref=self.source.at[rows] if own else at,
            dst_ref=at,
            send_sem=self.send_sem.at[(piece, lane) + index],
            recv_sem=self.recv_sem.at[(piece,) + index],
            device_id=peer(digit, offset),
            device_id_type=pl.DeviceIdType.MESH,
        )

    def send(self, piece, block, exists, digit, directions, tag, own=False):
        for way, (offset, has) in enumerate(moves(digit)):
            if directions is not None and way not in directions:
                continue
            copy = self.copy(piece, block, digit, offset, way, own)
            condition = both(exists, has)
            when(condition, copy.start)
            self.sent[(piece, tag, digit, way)] = (block, exists, own)

    def events(self, piece):
        order = self.pieces[piece][0]
        here = {d: place(d) for d in order}
        found = []

        def begin(after):
            for digit in order:
                self.send(piece, here, None, digit, None, (), own=True)

        found.append((0, begin, ()))

        def arrivals(stage, block, exists, tag, depth):
            digit = order[stage]
            for hop, travel, q, there in relatives(digit):
                source = {**block, digit: q}
                condition = both(exists, there)
                label = tag + ((digit, hop, travel),)

                def arrive(after, source=source, condition=condition, travel=travel, label=label):
                    offset, _ = moves(digit)[0]
                    when(condition, self.copy(piece, source, digit, offset, 0, False).wait_recv)
                    if digit[2] > 2:
                        self.send(piece, source, condition, digit, (0 if travel > 0 else 1,), label)
                    for later in order[stage + 1 :]:
                        self.send(piece, source, condition, later, None, label)
                    if after is not None:
                        after(piece, source, condition, label)

                found.append((depth + hop, arrive, label))

        def expand(stage, earlier, block, exists, tag, depth):
            if earlier == stage:
                arrivals(stage, block, exists, tag, depth)
                return
            digit = order[earlier]
            expand(stage, earlier + 1, {**block, digit: here[digit]}, exists, tag, depth)
            for hop, travel, q, there in relatives(digit):
                expand(
                    stage, earlier + 1, {**block, digit: q}, both(exists, there),
                    tag + ((digit, hop, travel),), depth + hop,
                )

        for stage in range(len(order)):
            expand(stage, 0, dict(here), None, (), 0)
        return found

    def queue(self):
        entries = []
        for piece in range(len(self.pieces)):
            for depth, action, tag in self.events(piece):
                entries.append((depth, piece, len(entries), action, tag))
        entries.sort(key=lambda entry: entry[:3])
        return [(piece, action, tag) for _, piece, _, action, tag in entries]

    def run(self, after=None):
        for _, action, _ in self.queue():
            action(after)

    def drain(self):
        for (piece, _, digit, way), (block, exists, own) in self.sent.items():
            offset, has = moves(digit)[way]
            copy = self.copy(piece, block, digit, offset, way, own)
            when(both(exists, has), copy.wait_send)


def gather_kernel(layout, pieces, x_ref, out_ref, send_sem, recv_sem, local_sem):
    barrier_all(layout)
    gather = Gather(layout, pieces, out_ref, x_ref, send_sem, recv_sem)
    gather.run()
    local = pltpu.make_async_copy(x_ref, out_ref.at[tuple(place(d) for d in layout)], local_sem)
    local.start()
    local.wait()
    gather.drain()


def pieces_of(rows, orders, chunks):
    units = max(1, rows // 16)
    chunks = min(chunks, units)
    cuts = [units * i // chunks * 16 for i in range(chunks)] + [rows]
    return [(orders[i % len(orders)], cuts[i], cuts[i + 1] - cuts[i]) for i in range(chunks)]


def events_of(order):
    total, held = 0, 1
    for digit in order:
        around = 1 if digit[2] == 2 else 2 * (digit[2] - 1)
        total += held * around
        held *= 1 + around
    return total


def gather(x, axes, layout, orders, chunks, ident, name):
    rows, columns = x.shape
    if rows % 16 or len(orders) * events_of(orders[0]) > 256:
        return lax.all_gather(x, axes, axis=0, tiled=True)
    pieces = pieces_of(rows, orders, chunks)
    dims = tuple(d[2] for d in layout)
    out = pl.pallas_call(
        functools.partial(gather_kernel, layout, pieces),
        out_shape=jax.ShapeDtypeStruct(dims + (rows, columns), x.dtype),
        in_specs=[pl.BlockSpec(memory_space=pltpu.VMEM)],
        out_specs=pl.BlockSpec(memory_space=pl.ANY),
        scratch_shapes=Gather.semaphores(layout, pieces) + [pltpu.SemaphoreType.DMA],
        compiler_params=pltpu.CompilerParams(collective_id=ident, has_side_effects=True),
        name=name,
    )(x)
    return out.reshape(math.prod(dims) * rows, columns)


def nt_dot(left, right):
    return lax.dot_general(
        left, right, (((1,), (1,)), ((), ())), preferred_element_type=jnp.float32
    )


def window_of(blocks):
    return blocks // 2 + 1


def gram_kernel(block, where_ref, x_ref, part_ref):
    blocks = x_ref.shape[0] // block
    mine = part_ref.shape[0] // block
    window = part_ref.shape[1] // block
    first = where_ref[0] * mine
    left_at = pl.ds(pl.multiple_of(first * block, block), mine * block)
    for j in range(mine + window - 1):
        low, high = max(0, j - window + 1), min(mine - 1, j)
        other = lax.rem(first + j, blocks)
        right = x_ref[pl.ds(pl.multiple_of(other * block, block), block), :]
        rows = pl.ds(
            pl.multiple_of((first + low) * block, block), (high - low + 1) * block
        )
        product = nt_dot(x_ref[rows, :], right).astype(jnp.bfloat16)
        for i in range(low, high + 1):
            at = (i - low) * block
            part_ref[i * block : (i + 1) * block, (j - i) * block : (j - i + 1) * block] = (
                product[at : at + block, :]
            )


def reduce_kernel(
    block, rows, pieces, far, near, x_ref, columns_ref, share_ref, held, part, got_near, half, got_far,
    send_sem, recv_sem, near_send, near_recv, far_send, far_recv, out_sem,
):
    order = pieces[0][0]
    layout = tuple(sorted(order, key=lambda d: -d[1]))
    shards = math.prod(d[2] for d in layout)
    mine = x_ref.shape[0] // block
    total = part.shape[0]
    window = total - mine + 1
    lines = far[2]
    axis = layout[0][0]
    shard = lax.axis_index(axis)
    barrier_lines(layout + (far, near))
    gather = Gather(layout, pieces, held, x_ref, send_sem, recv_sem)
    queue = gather.queue()
    events = [entry for entry in queue if entry[2]]

    def home(t, tag):
        for digit, _, _ in tag:
            _, stride, _, _ = digit
            t = t - stride if (t // stride) % 2 else t + stride
        return t

    arrival = list(range(total))

    def needed(t, j):
        s, piece = j // mine % shards, j % mine
        return {((t + s) % shards, piece)} if s else set()

    side, close = order

    def rank(t, e):
        piece, _, tag = events[e]
        if len(tag) == 2:
            kind = 1 if (t // close[1]) % 2 else 2
        else:
            kind = 0 if tag[0][0] == close else 2 if (t // close[1]) % 2 else 1
        return kind, piece

    turns = [sorted(range(len(events)), key=functools.partial(rank, t)) for t in range(shards)]

    slots = [[] for _ in range(total + 1)]
    done = [0] * shards
    early = []
    for k in range(total + 1):
        begun = {}
        for t in range(shards):
            last = len(events)
            if k < total:
                wanted = needed(t, arrival[k])
                last = max(
                    [done[t]]
                    + [
                        turn + 1
                        for turn, e in enumerate(turns[t])
                        if (home(t, events[e][2]), events[e][0]) in wanted
                    ]
                )
            if k == total - 1 and last == done[t]:
                early.append(t)
            for e in turns[t][done[t] : last]:
                begun.setdefault(e, []).append(t)
            done[t] = last
        slots[k] = sorted(begun.items())
    copies = {}

    def keep(piece, source, condition, tag):
        _, row, count = pieces[piece]
        at = tuple(source[d] for d in layout) + (pl.ds(row, count), slice(None))
        number = next(e for e, entry in enumerate(events) if entry[0] == piece and entry[2] == tag)
        copies[number] = at
        pltpu.make_async_copy(held.at[at], columns_ref.at[at], out_sem.at[number]).start()

    here = {d: place(d) for d in layout}
    ahead = here[close] == 0
    for piece in range(len(pieces)):
        gather.send(piece, here, ahead, side, None, (), own=True)
        gather.sent[(piece, (), side, 0)] = (here, None, True)
        gather.send(piece, here, None, close, None, (), own=True)
    own = pltpu.make_async_copy(
        x_ref, columns_ref.at[tuple(place(d) for d in layout)], out_sem.at[len(events)]
    )
    own.start()

    def handle(e):
        piece, action, tag = events[e]
        action(keep)
        last = len(pieces) - 1
        if len(tag) == 2 and piece >= last - 1:
            freed = range(1) if piece < last else range(1 if last else 0, last + 1)
            offset, _ = moves(side)[0]
            for p in freed:
                copy = gather.copy(p, here, side, offset, 0, True)
                pl.when(jnp.logical_not(ahead))(copy.start)

    def advance(d):
        for e, who in slots[d]:
            if len(who) == shards:
                handle(e)
            else:
                condition = functools.reduce(lambda a, b: a | b, [shard == t for t in who])
                pl.when(condition)(functools.partial(handle, e))

    def span(j):
        low, high = max(0, j - window + 1), min(mine - 1, j)
        return low, high - low + 1

    def near_copy(j):
        blocks = pl.ds(*span(j))
        return pltpu.make_async_remote_copy(
            src_ref=part.at[j, blocks, :, 1 - place(near)],
            dst_ref=got_near.at[j, blocks],
            send_sem=near_send.at[j],
            recv_sem=near_recv.at[j],
            device_id=peer(near, 1 - 2 * place(near)),
            device_id_type=pl.DeviceIdType.MESH,
        )

    def far_copy(j, step, arriving):
        there, offset = around(far, step)
        slot = there if arriving else place(far)
        blocks = pl.ds(*span(j))
        return pltpu.make_async_remote_copy(
            src_ref=half.at[j, there, blocks],
            dst_ref=got_far.at[j, slot, blocks],
            send_sem=far_send.at[j, there],
            recv_sem=far_recv.at[j, slot],
            device_id=peer(far, offset),
            device_id_type=pl.DeviceIdType.MESH,
        )

    def form(k):
        j = arrival[k]
        s, piece = j // mine % shards, j % mine
        at = (pl.ds(piece * block, block), slice(None))
        if s:
            other = lax.rem(shard + s, shards)
            at = tuple(lax.rem(lax.div(other, g[1]), g[2]) for g in layout) + at
            right = held[at]
        else:
            right = x_ref[at]
        low, size = span(j)
        product = nt_dot(x_ref[low * block : (low + size) * block, :], right).astype(jnp.bfloat16)
        for i in range(low, low + size):
            row = (i - low) * block
            part[j, i] = product[row : row + block, :].reshape(lines, near[2], rows, block)
        near_copy(j).start()

    def halve(j):
        low, size = span(j)
        near_copy(j).wait_recv()
        for i in range(low, low + size):
            for line in range(lines):
                half[j, line, i] = (
                    part[j, i, line, place(near)].astype(jnp.float32)
                    + got_near[j, i, line].astype(jnp.float32)
                ).astype(jnp.bfloat16)
        for step in range(1, lines):
            far_copy(j, step, False).start()

    def finish(j):
        low, size = span(j)
        for step in range(1, lines):
            far_copy(j, step, True).wait_recv()
        for i in range(low, low + size):
            value = half[j, place(far), i].astype(jnp.float32)
            for step in range(1, lines):
                there, _ = around(far, step)
                value = value + got_far[j, there, i].astype(jnp.float32)
            d = j - i
            share_ref[i * rows : (i + 1) * rows, d * block : (d + 1) * block] = value.astype(jnp.bfloat16)

    def among(who):
        return functools.reduce(lambda a, b: a | b, [shard == t for t in who])

    split = bool(early) and len(early) < shards
    for k in range(total):
        if k > 0:
            halve(arrival[k - 1])
        if k > 1:
            finish(arrival[k - 2])
        advance(k)
        if k == total - 1 and split:
            pl.when(jnp.logical_not(among(early)))(functools.partial(form, k))
        else:
            form(k)
        if k == total - 2 and split:
            pl.when(among(early))(functools.partial(form, total - 1))
    halve(arrival[total - 1])
    for j in arrival[-2:]:
        finish(j)
    advance(total)

    for j in range(total):
        near_copy(j).wait_send()
        for step in range(1, lines):
            far_copy(j, step, False).wait_send()
    for number, at in copies.items():
        pltpu.make_async_copy(held.at[at], columns_ref.at[at], out_sem.at[number]).wait()
    own.wait()
    gather.drain()


def reduced_gram(iterate, digits, block, window, ident):
    layout = tuple(digits["tp"])
    far, near = digits["mats"]
    mine, width = iterate.shape
    rows = block // (far[2] * near[2])
    order = tuple(sorted(layout, key=lambda d: d[3]))
    pieces = [(order, row, block) for row in range(0, mine, block)]
    dims = tuple(d[2] for d in layout)
    own = mine // block
    total, lines = window // block + own - 1, far[2]
    near_tile = pltpu.VMEM((total, own, lines, rows, block), jnp.bfloat16)
    far_tile = pltpu.VMEM((total, lines, own, rows, block), jnp.bfloat16)
    dma = pltpu.SemaphoreType.DMA
    blocks = math.prod(dims) - 1
    columns, share = pl.pallas_call(
        functools.partial(reduce_kernel, block, rows, pieces, far, near),
        out_shape=(
            jax.ShapeDtypeStruct(dims + iterate.shape, jnp.bfloat16),
            jax.ShapeDtypeStruct((own * rows, window), jnp.bfloat16),
        ),
        in_specs=[pl.BlockSpec(memory_space=pltpu.VMEM)],
        out_specs=(pl.BlockSpec(memory_space=pl.ANY), pl.BlockSpec(memory_space=pltpu.VMEM)),
        scratch_shapes=[
            pltpu.VMEM(dims + iterate.shape, jnp.bfloat16),
            pltpu.VMEM((total, own, lines, near[2], rows, block), jnp.bfloat16),
            near_tile, far_tile, far_tile,
        ]
        + Gather.semaphores(layout, pieces)
        + [dma((total,))] * 2
        + [dma((total, lines))] * 2
        + [dma((blocks * len(pieces) + 1,))],
        compiler_params=pltpu.CompilerParams(
            collective_id=ident, has_side_effects=True, vmem_limit_bytes=grant
        ),
        name="reduced_gram",
    )(iterate)
    return columns.reshape(dims[0] * math.prod(dims[1:]) * mine, width), share


def polynomial_rows(gram, own, one, two, left, right, raw, sums, scale, where_ref):
    size = gram.shape[0]
    count = own.shape[0]
    width = math.gcd(size, 1024)
    def columns(body):
        @pl.loop(0, size // width)
        def _(step):
            body(pl.ds(pl.multiple_of(step * width, width), width))

    if where_ref is None:
        pass
    elif count % 16 == 0:
        own[...] = gram[pl.ds(pl.multiple_of(where_ref[0] * count, 16), count), :]
    else:
        row = lax.broadcasted_iota(jnp.int32, (count, size), 0) + where_ref[0] * count
        column = lax.broadcasted_iota(jnp.int32, (count, size), 1)
        two[...] = (row == column).astype(jnp.float32).astype(jnp.bfloat16)

        def select(at):
            own[:, at] = jnp.dot(
                two[...], gram[:, at], preferred_element_type=jnp.float32
            ).astype(jnp.bfloat16)

        columns(select)

    tile = math.gcd(size, 512)

    @pl.loop(0, size // tile)
    def _(step):
        at = pl.ds(pl.multiple_of(step * tile, tile), tile)
        raw[:, at] = jnp.dot(own[...], gram[:, at], preferred_element_type=jnp.float32)
        sums[:, at] = jnp.sum(jnp.abs(gram[:, at].astype(jnp.float32)), axis=0, keepdims=True)

    bound = jnp.max(sums[...], axis=1, keepdims=True) + epsilon
    root = lax.rsqrt(jnp.broadcast_to(bound, (1, 128)))
    inverse = (root * root)[:, :1]

    def times_gram(source, at):
        return inverse * jnp.dot(source[...], gram[:, at], preferred_element_type=jnp.float32)

    def wide(ref, at):
        return ref[:, at].astype(jnp.float32)

    def apply(source, target, constant=None):
        def body(at):
            value = times_gram(source, at)
            if constant is not None:
                value = value + (constant * inverse) * wide(own, at)
            target[:, at] = value.astype(jnp.bfloat16)

        columns(body)

    def polynomial(source, middle, target):
        apply(source, middle)

        def body(at):
            target[:, at] = (
                first_coef * wide(source, at)
                + second_coef * wide(middle, at)
                + third_coef * times_gram(middle, at)
            ).astype(jnp.bfloat16)

        columns(body)

    def first(at):
        one[:, at] = (
            second_coef * (inverse * wide(own, at)) + third_coef * (inverse * (inverse * raw[:, at]))
        ).astype(jnp.bfloat16)

    columns(first)
    apply(one, left, first_coef)
    polynomial(left, right, two)
    polynomial(two, right, left)

    def keep(at):
        two[:, at] = left[:, at]

    columns(keep)
    apply(two, right)
    polynomial(right, left, own)
    polynomial(own, left, right)

    def finish(at):
        mixed = (
            first_coef * wide(one, at) + second_coef * wide(two, at) + third_coef * wide(right, at)
        )
        left[:, at] = ((scale * root[:, :1]) * mixed).astype(jnp.bfloat16)

    columns(finish)
    return root


def poly_kernel(block, scale, where_ref, compact_ref, out_ref, kappa_ref, gram, own, one, two, left, right, raw, sums):
    size = gram.shape[0]
    blocks = size // block
    window = compact_ref.shape[1] // block
    for i in range(blocks):
        for d in range(window):
            j = (i + d) % blocks
            tile = compact_ref[i * block : (i + 1) * block, d * block : (d + 1) * block]
            gram[i * block : (i + 1) * block, j * block : (j + 1) * block] = tile
            if d > 0 and 2 * d != blocks:
                gram[j * block : (j + 1) * block, i * block : (i + 1) * block] = tile.T

    root = polynomial_rows(gram, own, one, two, left, right, raw, sums, scale, where_ref)
    kappa_ref[...] = (scale * first_coef * first_coef) * root
    out_ref[...] = left[...]


def finish_kernel(
    block, scale, layout, pieces, near_pieces, share_ref, columns_ref, out_ref, held, gram, own, one, two, left,
    right, raw, sums, rows, columns, result, send_sem, recv_sem, rows_send, rows_recv, in_sem, out_sem,
):
    barrier_all(layout)
    tp = tuple(d for d in layout if d[0] == "tp")
    far, near = (d for d in layout if d[0] == "mats")
    load = pltpu.make_async_copy(columns_ref, columns, in_sem)
    gather = Gather(layout, pieces, held, share_ref, send_sem, recv_sem)
    queue = gather.queue()
    for _, action, tag in queue:
        if not tag:
            action(None)
    load.start()
    held[tuple(place(d) for d in layout)] = share_ref[...]
    for _, action, tag in queue:
        if tag:
            action(None)

    size = gram.shape[0]
    count, window = share_ref.shape
    blocks = size // block
    shards = math.prod(d[2] for d in tp)
    mine = size // shards
    own_blocks = mine // block
    seg = count // own_blocks
    for t in range(shards):
        at = tuple((t // d[1]) % d[2] for d in tp)
        for d in range(window // block):
            for k in range(own_blocks):
                i = t * own_blocks + k
                j = (i + d) % blocks
                tile = held[at + (slice(None), slice(None), pl.ds(k * seg, seg), pl.ds(d * block, block))]
                tile = tile.reshape(block, block)
                gram[i * block : (i + 1) * block, j * block : (j + 1) * block] = tile
                if d > 0 and 2 * d != blocks:
                    gram[j * block : (j + 1) * block, i * block : (i + 1) * block] = tile.T

    first = lax.axis_index("tp") * mine + lax.axis_index("mats") * seg
    for k in range(own_blocks):
        at = pl.ds(pl.multiple_of(first + k * block, 16), seg)
        own[k * seg : (k + 1) * seg, :] = gram[at, :]
    root = polynomial_rows(gram, own, one, two, left, right, raw, sums, scale, None)
    kappa = ((scale * first_coef * first_coef) * root)[:, :1]

    spread = Gather((far, near), near_pieces, rows, left, rows_send, rows_recv)
    queue = spread.queue()
    for _, action, tag in queue:
        if not tag:
            action(None)
    rows[place(far), place(near)] = left[...]
    load.wait()
    pair = near[2] * count
    width = math.gcd(columns.shape[1], 512)
    shard_row = lax.axis_index("tp") * mine

    def multiply(line):
        matrix = rows[line].reshape(pair, size)

        @pl.loop(0, columns.shape[1] // width)
        def _(step):
            across = pl.ds(pl.multiple_of(step * width, width), width)
            product = jnp.dot(matrix, columns[:, across], preferred_element_type=jnp.float32)
            for n in range(near[2]):
                for k in range(own_blocks):
                    start = shard_row + k * block + (line * near[2] + n) * seg
                    mirror = columns[pl.ds(pl.multiple_of(start, 16), seg), across]
                    row = n * count + k * seg
                    result[k, line, n * seg : (n + 1) * seg, across] = (
                        product[row : row + seg, :] + kappa * mirror.astype(jnp.float32)
                    ).astype(jnp.bfloat16)

        pltpu.make_async_copy(result.at[:, line], out_ref.at[:, line], out_sem.at[line]).start()

    groups = [(None, place(far), None)]
    groups += [((far, hop, travel), q, there) for hop, travel, q, there in relatives(far)]
    missing = []
    for label, q, there in groups:
        wanted = set()
        for piece, _, tag in queue:
            if tag and [part for part in tag if part[0] == far] == ([label] if label else []):
                wanted.add((piece, tag))
        missing.append((wanted, q, there))
    for piece, action, tag in queue:
        if not tag:
            continue
        action(None)
        for wanted, q, there in missing:
            if (piece, tag) in wanted:
                wanted.remove((piece, tag))
                if not wanted:
                    when(there, functools.partial(multiply, q))
    for line in range(far[2]):
        pltpu.make_async_copy(result.at[:, line], out_ref.at[:, line], out_sem.at[line]).wait()
    gather.drain()
    spread.drain()


def finished(share, columns, digits, block, scale, ident):
    layout, _ = orders_of(digits)
    count, window = share.shape
    far, near = digits["mats"]
    side = [d for d in digits["tp"] if not d[3]]
    close = tuple(d for d in digits["tp"] if d[3])
    orders = [(far, near, side[0]) + close, (far, side[0], near) + close]
    pieces = pieces_of(count, orders, 2)
    most = (count * 5 // 6 + 15) // 16 * 16
    near_pieces = [((far, near), 0, most)]
    if most < count:
        near_pieces.append(((near, far), most, count - most))
    size, width = columns.shape
    dims = tuple(d[2] for d in layout)
    mine = count * far[2] * near[2]
    thin = pltpu.VMEM((count, size), jnp.bfloat16)
    shape = (mine // block, far[2], block // far[2], width)
    return pl.pallas_call(
        functools.partial(finish_kernel, block, scale, layout, pieces, near_pieces),
        out_shape=jax.ShapeDtypeStruct(shape, jnp.bfloat16),
        in_specs=[pl.BlockSpec(memory_space=pltpu.VMEM), pl.BlockSpec(memory_space=pl.ANY)],
        out_specs=pl.BlockSpec(memory_space=pl.ANY),
        scratch_shapes=[
            pltpu.VMEM(dims + share.shape, jnp.bfloat16),
            pltpu.VMEM((size, size), jnp.bfloat16),
        ]
        + [thin] * 5
        + [
            pltpu.VMEM((count, size), jnp.float32),
            pltpu.VMEM((1, size), jnp.float32),
            pltpu.VMEM((far[2], near[2], count, size), jnp.bfloat16),
            pltpu.VMEM((size, width), jnp.bfloat16),
            pltpu.VMEM(shape, jnp.bfloat16),
        ]
        + Gather.semaphores(layout, pieces)
        + Gather.semaphores((far, near), near_pieces)
        + [pltpu.SemaphoreType.DMA, pltpu.SemaphoreType.DMA((far[2],))],
        compiler_params=pltpu.CompilerParams(
            collective_id=ident, has_side_effects=True, vmem_limit_bytes=63 * 1024 * 1024
        ),
        name="finished",
    )(share, columns).reshape(mine, width)


def paired(digits, block):
    tp, mats = digits["tp"], digits["mats"]
    if len(tp) != 2 or len(mats) != 2 or mats[1][2] != 2 or any(d[2] != 2 for d in tp):
        return False
    if tp[0][3] or not tp[1][3]:
        return False
    return block % (16 * mats[0][2] * mats[1][2]) == 0


def orders_of(digits):
    layout = tuple(digits["tp"]) + tuple(digits["mats"])
    far = {axis: [d for d in found if not d[3]] for axis, found in digits.items()}
    near = [d for d in layout if d[3]]
    one = tuple(far["mats"] + far["tp"] + near)
    two = tuple(far["mats"][:1] + far["tp"] + far["mats"][1:] + near)
    return layout, [one, two] if one != two else [one]


def per_device(scale, digits, grad, momentum):
    new_momentum = momentum_beta * momentum + grad.astype(jnp.float32)
    iterate = (grad.astype(jnp.float32) + momentum_beta * new_momentum).astype(jnp.bfloat16)
    layout, orders = orders_of(digits)
    lines = {axis: tuple(sorted(found, key=lambda d: d[3])) for axis, found in digits.items()}
    size = momentum.shape[0] * lax.axis_size("tp")
    mine = iterate.shape[0]
    block = math.gcd(mine, 256)
    window = window_of(size // block) * block
    smem = pl.BlockSpec(memory_space=pltpu.SMEM)
    whole = pl.BlockSpec(memory_space=pltpu.VMEM)
    params = pltpu.CompilerParams(vmem_limit_bytes=grant)
    tp = lax.axis_index("tp")
    if paired(digits, block):
        columns, share = reduced_gram(iterate, digits, block, window, 1)
        return (finished(share, columns, digits, block, scale, 2), new_momentum)
    columns = gather(iterate, "tp", tuple(digits["tp"]), [lines["tp"]], 6, 1, "gather_x")
    part = pl.pallas_call(
        functools.partial(gram_kernel, block),
        out_shape=jax.ShapeDtypeStruct((mine, window), jnp.bfloat16),
        in_specs=[smem, whole],
        out_specs=whole,
        compiler_params=params,
        name="gram",
    )(tp.reshape(1), columns)
    share = lax.psum_scatter(part, "mats", scatter_dimension=0, tiled=True)
    compact = gather(share, ("tp", "mats"), layout, orders, 2, 2, "gather_gram")
    count = share.shape[0]
    place = tp * lax.axis_size("mats") + lax.axis_index("mats")
    thin = pltpu.VMEM((count, size), jnp.bfloat16)
    rows, kappa = pl.pallas_call(
        functools.partial(poly_kernel, block, scale),
        out_shape=(
            jax.ShapeDtypeStruct((count, size), jnp.bfloat16),
            jax.ShapeDtypeStruct((1, 128), jnp.float32),
        ),
        in_specs=[smem, whole],
        out_specs=(whole, whole),
        scratch_shapes=[pltpu.VMEM((size, size), jnp.bfloat16)]
        + [thin] * 5
        + [pltpu.VMEM((count, size), jnp.float32), pltpu.VMEM((1, size), jnp.float32)],
        compiler_params=params,
        cost_estimate=pl.CostEstimate(
            flops=22 * count * size * size, bytes_accessed=size * window * 2, transcendentals=0
        ),
        name="poly",
    )(place.reshape(1), compact)
    matrix = gather(rows, "mats", tuple(digits["mats"]), [lines["mats"]], 3, 3, "gather_rows")
    product = jnp.dot(matrix, columns, preferred_element_type=jnp.float32)
    update = (product + kappa[0, 0] * iterate.astype(jnp.float32)).astype(jnp.bfloat16)
    return (update, new_momentum)


def solution(mesh):
    digits = digits_of(mesh)

    def step(grad, momentum):
        scale = shape_gain * math.sqrt(max(grad.shape))
        return jax.shard_map(
            functools.partial(per_device, scale, digits),
            mesh=mesh,
            in_specs=(P("tp", "mats"), P("tp", "mats")),
            out_specs=(P("tp", "mats"), P("tp", "mats")),
            check_vma=False,
        )(grad, momentum)

    return step
```
